16 devices in a mesh: vp: 16 (over z, y, x, core).
Axes of the slice: x: 2, y: 2, z: 2, core: 2. Of those that a mesh axis runs over, the one named last changes fastest.
Arguments:
- table_in: float32 [32000, 2048], P('vp')
- table_out: float32 [32000, 2048], P('vp')
- center_ids: int32 [32768], P('vp')
- context_ids: int32 [32768], P('vp')
- negative_ids: int32 [16384], P('vp')
Outputs:
- output 1: float32 [32000, 2048], P('vp')
- output 2: float32 [32000, 2048], P('vp')
All inputs are finite; a program needn't handle non-finite values.
Results may differ from the reference program's by a relative error of at most 0.001.
Values sent between devices are 32-bit elements.
A program may use at most 1 GiB of HBM per device.

```python
import jax
import jax.numpy as jnp
from jax import lax

VOCAB_SIZE = 32000
EMBED_DIM = 2048
PAIRS_DEV = 2048
NEGATIVES = 1024
SHARDS = 16
ROWS_SHARD = VOCAB_SIZE // SHARDS
NEG_WEIGHT = 5.0
LEARN_RATE = 1.0
NEG_SCALE = NEG_WEIGHT / NEGATIVES


def draw_ids(base_key, num_ids):
    common_slots = 3 * num_ids // SHARDS
    common_rows = common_slots // 4
    span_rows = ROWS_SHARD - common_rows
    key_common, key_start, key_perm = jax.random.split(base_key, 3)
    slot_idx = jnp.arange(num_ids, dtype=jnp.int32)
    common_pick = jax.random.randint(key_common, (SHARDS, num_ids), 0, common_rows, dtype=jnp.int32)
    common_part = jnp.where(slot_idx < common_rows, slot_idx, common_pick)
    other_idx = jnp.maximum(slot_idx - common_slots, 0)
    shard_idx = other_idx % SHARDS
    rank_idx = other_idx // SHARDS
    starts = jax.random.randint(key_start, (SHARDS, SHARDS), 0, span_rows, dtype=jnp.int32)
    other_part = shard_idx * ROWS_SHARD + common_rows + (starts[:, shard_idx] + rank_idx) % span_rows
    id_table = jnp.where(slot_idx < common_slots, common_part, other_part)
    return jax.random.permutation(key_perm, id_table, axis=1, independent=True).reshape(-1)


def setup_inputs(seed: int = 0) -> dict:
    base_key = jax.random.key(seed)
    key_in, key_out, key_center, key_context, key_neg = jax.random.split(base_key, 5)
    row_scale = EMBED_DIM ** -0.25
    table_in = jax.random.normal(key_in, (VOCAB_SIZE, EMBED_DIM), jnp.float32) * row_scale
    table_out = jax.random.normal(key_out, (VOCAB_SIZE, EMBED_DIM), jnp.float32) * row_scale
    return {'table_in': table_in, 'table_out': table_out, 'center_ids': draw_ids(key_center, PAIRS_DEV), 'context_ids': draw_ids(key_context, PAIRS_DEV), 'negative_ids': draw_ids(key_neg, NEGATIVES)}


def reference(table_in, table_out, center_ids, context_ids, negative_ids):
    zero_table = jnp.zeros((VOCAB_SIZE, EMBED_DIM), jnp.float32)

    def scan_body(state_in, batch_ids):
        grad_in, grad_out = state_in
        center_row, context_row, negative_row = batch_ids
        center_vec = jnp.take(table_in, center_row, axis=0)
        context_vec = jnp.take(table_out, context_row, axis=0)
        negative_vec = jnp.take(table_out, negative_row, axis=0)
        pos_score = jnp.sum(center_vec * context_vec, axis=1)
        center_half = center_vec.astype(jnp.bfloat16)
        negative_half = negative_vec.astype(jnp.bfloat16)
        neg_score = jnp.dot(center_half, negative_half.T, preferred_element_type=jnp.float32)
        pos_grad = (jax.nn.sigmoid(pos_score) - 1.0)[:, None]
        neg_grad = (NEG_SCALE * jax.nn.sigmoid(neg_score)).astype(jnp.bfloat16)
        d_center = pos_grad * context_vec + jnp.dot(neg_grad, negative_half, preferred_element_type=jnp.float32)
        d_context = pos_grad * center_vec
        d_negative = jnp.dot(neg_grad.T, center_half, preferred_element_type=jnp.float32)
        grad_in = grad_in.at[center_row].add(d_center)
        grad_out = grad_out.at[context_row].add(d_context).at[negative_row].add(d_negative)
        return (grad_in, grad_out), None

    start_state = (zero_table, zero_table)
    batches = (center_ids.reshape(SHARDS, PAIRS_DEV), context_ids.reshape(SHARDS, PAIRS_DEV), negative_ids.reshape(SHARDS, NEGATIVES))
    grad_in, grad_out = lax.scan(scan_body, start_state, batches)[0]
    return (table_in - LEARN_RATE * grad_in, table_out - LEARN_RATE * grad_out)
```

```python
import jax
import jax.numpy as jnp
from jax import lax
from jax.sharding import PartitionSpec as P

LEARN_RATE = 1.0
NEG_WEIGHT = 5.0
AXIS_NAME = 'vp'
TILE = 8
LANES = 128
SLOT_BLOCKS = 16


def up8(count):
    return (count + 7) // 8 * 8


def distinct_bound(num_ids, shards):
    common_slots = 3 * num_ids // shards
    return common_slots // 4 + (num_ids - common_slots + shards - 1) // shards


def onehot(values, size):
    return (values[:, None] == lax.broadcasted_iota(jnp.int32, (1, size), 1)).astype(jnp.bfloat16)


def dot_f32(a, b, dims):
    return lax.dot_general(a, b, (dims, ((), ())), preferred_element_type=jnp.float32)


def request_layout(id_list, shard_rows, shards, capacity):
    hot = id_list < shards * TILE
    owner = jnp.where(hot, id_list // TILE, id_list // shard_rows)
    slot = jnp.where(hot, id_list % TILE, id_list % shard_rows + TILE)
    high = onehot(owner * SLOT_BLOCKS + slot // LANES, shards * SLOT_BLOCKS)
    low = onehot(slot % LANES, LANES)
    count = dot_f32(high, low, ((0,), (0,)))
    shape = (shards * SLOT_BLOCKS, LANES)
    row_idx = lax.broadcasted_iota(jnp.int32, shape, 0)
    lane_idx = lax.broadcasted_iota(jnp.int32, shape, 1)
    lent = (row_idx % SLOT_BLOCKS == 0) & (lane_idx < TILE)
    present = (count > 0.0) | lent
    ones = present.astype(jnp.bfloat16)
    upper = (lax.broadcasted_iota(jnp.int32, (LANES, LANES), 0) <= lax.broadcasted_iota(jnp.int32, (LANES, LANES), 1)).astype(jnp.bfloat16)
    inclusive = dot_f32(ones, upper, ((1,), (0,)))
    block_total = jnp.sum(present.astype(jnp.float32), axis=1).reshape(shards, SLOT_BLOCKS)
    before = (lax.broadcasted_iota(jnp.int32, (SLOT_BLOCKS, SLOT_BLOCKS), 0) < lax.broadcasted_iota(jnp.int32, (SLOT_BLOCKS, SLOT_BLOCKS), 1))
    block_start = dot_f32(block_total.astype(jnp.bfloat16), before.astype(jnp.bfloat16), ((1,), (0,)))
    rank = inclusive - ones.astype(jnp.float32) + block_start.reshape(-1)[:, None]
    largest = jnp.max(jnp.sum(block_total, axis=1)).astype(jnp.int32)
    rank_of_id = jnp.sum(dot_f32(high, rank.astype(jnp.bfloat16), ((1,), (0,))) * low.astype(jnp.float32), axis=1).astype(jnp.int32)
    rank_or_none = jnp.where(present, rank, -1.0).reshape(shards, 1, SLOT_BLOCKS * LANES)
    cells = lax.broadcasted_iota(jnp.int32, (1, capacity, 1), 1).astype(jnp.float32)
    slots = lax.broadcasted_iota(jnp.int32, (1, 1, SLOT_BLOCKS * LANES), 2).astype(jnp.float32)
    slot_of_cell = jnp.sum(jnp.where(rank_or_none == cells, slots + 1.0, 0.0), axis=2).astype(jnp.int32) - 1
    return owner, rank_of_id, slot_of_cell, largest


def exchange(blocks):
    return lax.all_to_all(blocks, AXIS_NAME, 0, 0)


def take_rows(rows, idx):
    return rows.at[idx].get(mode='promise_in_bounds')


def solution(mesh):
    shards = mesh.shape[AXIS_NAME]

    def device_step(in_shard, out_shard, center_ids, context_ids, negative_ids):
        shard_rows, depth = in_shard.shape
        num_negs = negative_ids.shape[0]
        lists = (center_ids, context_ids, negative_ids)
        full = tuple(up8(distinct_bound(ids.shape[0], shards) + TILE) for ids in lists)
        usual = tuple(up8(TILE + ids.shape[0] * 13 // (16 * shards)) for ids in lists)
        me = lax.axis_index(AXIS_NAME)

        lent_rows = shards * TILE
        lent = jnp.concatenate([in_shard[:lent_rows].reshape(shards, TILE, depth), out_shard[:lent_rows].reshape(shards, TILE, depth)], axis=1)
        lent_here = exchange(lent)[0]
        hot_in, hot_out = lent_here[:TILE], lent_here[TILE:]

        owners, ranks, asks, largest = zip(*(request_layout(ids, shard_rows, shards, cap) for ids, cap in zip(lists, full)))
        head = jnp.broadcast_to(jnp.stack(largest)[None, :], (shards, 3))
        arrived = exchange(jnp.concatenate(asks + (head,), axis=1))
        edge1, edge2, edge3 = full[0], full[0] + full[1], sum(full)
        slots = (arrived[:, :edge1], arrived[:, edge1:edge2], arrived[:, edge2:edge3])
        most = jnp.max(arrived[:, edge3:], axis=0)
        unit = jnp.where(most[2] >= 0, 1.0, 0.0)
        fits = jnp.all(most <= jnp.array(usual, jnp.int32))

        def run(caps, in_shard, out_shard, hot_in, hot_out, owners, ranks, slots, unit):
            cell_of_id = [owner * cap + rank for owner, rank, cap in zip(owners, ranks, caps)]
            asked = [slot[:, :cap] for slot, cap in zip(slots, caps)]

            def fetch(table, hot_rows, slot):
                rows = take_rows(table, jnp.maximum(slot - TILE, 0))
                rows = lax.dynamic_update_slice(rows, jnp.broadcast_to(hot_rows[None], (shards, TILE, depth)), (0, 0, 0))
                return exchange(rows).reshape(-1, depth)

            in_rows = fetch(in_shard, hot_in, asked[0])
            neg_rows = fetch(out_shard, hot_out, asked[2])
            ctx_rows = fetch(out_shard, hot_out, asked[1])

            center_vec = take_rows(in_rows, cell_of_id[0])
            negative_vec = take_rows(neg_rows, cell_of_id[2])
            center_half = center_vec.astype(jnp.bfloat16)
            negative_half = (negative_vec * unit).astype(jnp.bfloat16)
            neg_score = dot_f32(center_half, negative_half, ((1,), (1,)))
            neg_grad = ((NEG_WEIGHT / num_negs) * jax.nn.sigmoid(neg_score)).astype(jnp.bfloat16)
            d_negative = -dot_f32(neg_grad, center_half, ((0,), (0,)))
            d_center_neg = dot_f32(neg_grad, negative_half, ((1,), (0,)))

            context_vec = take_rows(ctx_rows, cell_of_id[1])
            pos_grad = (jax.nn.sigmoid(jnp.sum(center_vec * context_vec, axis=1)) - 1.0)[:, None]
            d_context = -(pos_grad * center_vec)
            d_center = -(pos_grad * context_vec + d_center_neg)

            def send_back(grads, cells, cap):
                summed = jnp.zeros((shards * cap, depth), jnp.float32).at[cells].add(grads, mode='promise_in_bounds')
                return exchange(summed.reshape(shards, cap, depth))

            neg_back = send_back(d_negative, cell_of_id[2], caps[2])
            ctx_back = send_back(d_context, cell_of_id[1], caps[1])
            in_back = send_back(d_center, cell_of_id[0], caps[0])

            def apply(table, slot, grads):
                row = jnp.where(slot < TILE, shard_rows, slot - TILE)
                return table.at[row.reshape(-1)].add(LEARN_RATE * grads.reshape(-1, depth), mode='drop')

            def return_hot(table, hot_sum):
                total = lax.all_gather(hot_sum, AXIS_NAME, axis=0, tiled=True)
                return table.at[:lent_rows].add(jnp.where(me == 0, LEARN_RATE * total, 0.0))

            new_out = apply(apply(out_shard, asked[2], neg_back), asked[1], ctx_back)
            new_out = return_hot(new_out, jnp.sum(neg_back[:, :TILE], axis=0) + jnp.sum(ctx_back[:, :TILE], axis=0))
            new_in = return_hot(apply(in_shard, asked[0], in_back), jnp.sum(in_back[:, :TILE], axis=0))
            return new_in, new_out

        args = (in_shard, out_shard, hot_in, hot_out, owners, ranks, slots, unit)
        return lax.cond(fits, lambda *a: run(usual, *a), lambda *a: run(full, *a), *args)

    return jax.shard_map(device_step, mesh=mesh, in_specs=(P(AXIS_NAME, None), P(AXIS_NAME, None), P(AXIS_NAME), P(AXIS_NAME), P(AXIS_NAME)), out_specs=(P(AXIS_NAME, None), P(AXIS_NAME, None)), check_vma=False)
```

```python
import functools

import jax
import jax.numpy as jnp
from jax import lax
from jax.experimental import pallas as pl
from jax.experimental.pallas import tpu as pltpu
from jax.sharding import PartitionSpec as P

LEARN_RATE = 1.0
NEG_WEIGHT = 5.0
AXIS_NAME = 'vp'
TILE = 8
LANES = 128
SLOT_BLOCKS = 16
HEADER = 8


def up8(count):
    return (count + 7) // 8 * 8


def distinct_bound(num_ids, shards):
    common_slots = 3 * num_ids // shards
    return common_slots // 4 + (num_ids - common_slots + shards - 1) // shards


def onehot(values, size):
    return (values[:, None] == lax.broadcasted_iota(jnp.int32, (1, size), 1)).astype(jnp.bfloat16)


def dot_f32(a, b, dims):
    return lax.dot_general(a, b, (dims, ((), ())), preferred_element_type=jnp.float32)


def request_layout(id_list, shard_rows, shards, capacity):
    hot = id_list < shards * TILE
    owner = jnp.where(hot, id_list // TILE, id_list // shard_rows)
    slot = jnp.where(hot, id_list % TILE, id_list % shard_rows + TILE)
    high = onehot(owner * SLOT_BLOCKS + slot // LANES, shards * SLOT_BLOCKS)
    low = onehot(slot % LANES, LANES)
    count = dot_f32(high, low, ((0,), (0,)))
    shape = (shards * SLOT_BLOCKS, LANES)
    row_idx = lax.broadcasted_iota(jnp.int32, shape, 0)
    lane_idx = lax.broadcasted_iota(jnp.int32, shape, 1)
    lent = (row_idx % SLOT_BLOCKS == 0) & (lane_idx < TILE)
    present = (count > 0.0) | lent
    ones = present.astype(jnp.bfloat16)
    upper = (lax.broadcasted_iota(jnp.int32, (LANES, LANES), 0) <= lax.broadcasted_iota(jnp.int32, (LANES, LANES), 1)).astype(jnp.bfloat16)
    inclusive = dot_f32(ones, upper, ((1,), (0,)))
    block_total = jnp.sum(present.astype(jnp.float32), axis=1).reshape(shards, SLOT_BLOCKS)
    before = (lax.broadcasted_iota(jnp.int32, (SLOT_BLOCKS, SLOT_BLOCKS), 0) < lax.broadcasted_iota(jnp.int32, (SLOT_BLOCKS, SLOT_BLOCKS), 1))
    block_start = dot_f32(block_total.astype(jnp.bfloat16), before.astype(jnp.bfloat16), ((1,), (0,)))
    rank = inclusive - ones.astype(jnp.float32) + block_start.reshape(-1)[:, None]
    largest = jnp.max(jnp.sum(block_total, axis=1)).astype(jnp.int32)
    rank_of_id = jnp.sum(dot_f32(high, rank.astype(jnp.bfloat16), ((1,), (0,))) * low.astype(jnp.float32), axis=1).astype(jnp.int32)
    rank_or_none = jnp.where(present, rank, -1.0).reshape(shards, 1, SLOT_BLOCKS * LANES)
    cells = lax.broadcasted_iota(jnp.int32, (1, capacity, 1), 1).astype(jnp.float32)
    slots = lax.broadcasted_iota(jnp.int32, (1, 1, SLOT_BLOCKS * LANES), 2).astype(jnp.float32)
    slot_of_cell = jnp.sum(jnp.where(rank_or_none == cells, slots + 1.0, 0.0), axis=2).astype(jnp.int32) - 1
    return owner, rank_of_id, slot_of_cell, largest


def exchange(blocks):
    return lax.all_to_all(blocks, AXIS_NAME, 0, 0)


def take_rows(rows, idx):
    return rows.at[idx].get(mode='promise_in_bounds')


def meet(me, shards):
    barrier = pltpu.get_barrier_semaphore()
    for step in range(1, shards):
        pl.semaphore_signal(barrier, inc=1, device_id=(lax.rem(me + step, shards),), device_id_type=pl.DeviceIdType.MESH)
    pl.semaphore_wait(barrier, shards - 1)


def remote(src, dst, send_sem, recv_sem, peer):
    return pltpu.make_async_remote_copy(src_ref=src, dst_ref=dst, send_sem=send_sem, recv_sem=recv_sem, device_id=(peer,), device_id_type=pl.DeviceIdType.MESH)


def ask_kernel(shards, ask, in_shard, out_shard, got, lent_in, lent_out, ask_send, ask_recv, lend_send, lend_recv, own_sem):
    me = lax.axis_index(AXIS_NAME)
    meet(me, shards)

    def lend(peer, part):
        table, lent = ((in_shard, lent_in), (out_shard, lent_out))[part]
        return remote(table.at[pl.ds(pl.multiple_of(peer * TILE, TILE), TILE)], lent, lend_send.at[part, peer], lend_recv.at[part], peer)

    @pl.when(me == 0)
    def _():
        for peer in range(1, shards):
            lend(peer, 0).start()
            lend(peer, 1).start()
        pltpu.make_async_copy(in_shard.at[pl.ds(0, TILE)], lent_in, own_sem.at[0]).start()
        pltpu.make_async_copy(out_shard.at[pl.ds(0, TILE)], lent_out, own_sem.at[1]).start()

    copies = []
    for step in range(1, shards):
        peer = lax.rem(me + step, shards)
        copies.append(remote(ask.at[peer], got.at[me], ask_send.at[step], ask_recv.at[step], peer))
        copies[-1].start()
    got[me] = ask[me]
    for copy in copies:
        copy.wait()

    @pl.when(me == 0)
    def _():
        for peer in range(1, shards):
            lend(peer, 0).wait_send()
            lend(peer, 1).wait_send()
        pltpu.make_async_copy(in_shard.at[pl.ds(0, TILE)], lent_in, own_sem.at[0]).wait()
        pltpu.make_async_copy(out_shard.at[pl.ds(0, TILE)], lent_out, own_sem.at[1]).wait()

    @pl.when(me != 0)
    def _():
        lend(me, 0).wait_recv()
        lend(me, 1).wait_recv()


def ask_owners(ask, in_shard, out_shard, shards):
    depth = in_shard.shape[1]
    any_space, vmem = pl.BlockSpec(memory_space=pl.ANY), pl.BlockSpec(memory_space=pltpu.VMEM)
    tile = jax.ShapeDtypeStruct((TILE, depth), jnp.float32)
    return pl.pallas_call(
        functools.partial(ask_kernel, shards),
        out_shape=(jax.ShapeDtypeStruct(ask.shape, jnp.int32), tile, tile),
        in_specs=[vmem, any_space, any_space],
        out_specs=(vmem, vmem, vmem),
        scratch_shapes=[pltpu.SemaphoreType.DMA((shards,)), pltpu.SemaphoreType.DMA((shards,)), pltpu.SemaphoreType.DMA((2, shards)), pltpu.SemaphoreType.DMA((2,)), pltpu.SemaphoreType.DMA((2,))],
        compiler_params=pltpu.CompilerParams(collective_id=0, has_side_effects=True),
        name='ask_owners',
    )(ask, in_shard, out_shard)


def collect_kernel(shards, mine, got, send_sem, recv_sem):
    me = lax.axis_index(AXIS_NAME)
    ready = pltpu.get_barrier_semaphore()

    @pl.when(me == 0)
    def _():
        for peer in range(1, shards):
            pl.semaphore_signal(ready, inc=1, device_id=(peer,), device_id_type=pl.DeviceIdType.MESH)
        got[0] = mine[...]
        for peer in range(1, shards):
            remote(mine, got.at[peer], send_sem, recv_sem.at[peer], 0).wait_recv()

    @pl.when(me != 0)
    def _():
        pl.semaphore_wait(ready, 1)
        got[...] = jnp.zeros_like(got)
        copy = remote(mine, got.at[me], send_sem, recv_sem.at[me], 0)
        copy.start()
        copy.wait_send()


def collect_lent(mine, shards):
    vmem = pl.BlockSpec(memory_space=pltpu.VMEM)
    got = pl.pallas_call(
        functools.partial(collect_kernel, shards),
        out_shape=jax.ShapeDtypeStruct((shards,) + mine.shape, jnp.float32),
        in_specs=[vmem],
        out_specs=vmem,
        scratch_shapes=[pltpu.SemaphoreType.DMA, pltpu.SemaphoreType.DMA((shards,))],
        compiler_params=pltpu.CompilerParams(collective_id=1, has_side_effects=True),
        name='collect_lent',
    )(mine)
    return got.reshape(-1, mine.shape[1])


GROUP = 4
BUFFERS = 4


def apply_kernel(shards, caps, num_rows, *refs):
    lists = len(caps)
    rows, (lent, table), grads, out = refs[:lists], refs[lists:lists + 2], refs[lists + 2:2 * lists + 2], refs[2 * lists + 2]
    total, buf, load_sem, grad_sem, store_sem = refs[2 * lists + 3:]
    load = pltpu.make_async_copy(table, total.at[pl.ds(0, num_rows)], load_sem)
    load.start()

    def copy(i, source):
        place = lax.rem(source, BUFFERS)
        return pltpu.make_async_copy(grads[i].at[source], buf.at[place, pl.ds(0, caps[i])], grad_sem.at[place])

    for i in range(lists):
        for source in range(BUFFERS - 1):
            copy(i, source).start()
        if i == 0:
            load.wait()
            total[pl.ds(0, lent.shape[0]), :] += lent[...]

        def from_source(source, carry):
            @pl.when(source + BUFFERS - 1 < shards)
            def _():
                copy(i, source + BUFFERS - 1).start()

            copy(i, source).wait()
            place = lax.rem(source, BUFFERS)

            def group(number, carry):
                base = source * caps[i] + number * GROUP
                idx = [rows[i][base + k] for k in range(GROUP)]
                sums = [total[pl.ds(idx[k], 1), :] + buf[place, pl.ds(number * GROUP + k, 1), :] for k in range(GROUP)]
                for k in range(GROUP):
                    total[pl.ds(idx[k], 1), :] = sums[k]
                return carry

            return lax.fori_loop(TILE // GROUP, caps[i] // GROUP, group, carry)

        lax.fori_loop(0, shards, from_source, 0)
    store = pltpu.make_async_copy(total.at[pl.ds(0, num_rows)], out, store_sem)
    store.start()
    store.wait()


def apply_rows(table, lent, slots, grads):
    num_rows, depth = table.shape
    shards = grads[0].shape[0]
    caps = tuple(g.shape[1] for g in grads)
    rows = [jnp.where(slot < TILE, num_rows, slot - TILE).reshape(-1) for slot in slots]
    any_space = pl.BlockSpec(memory_space=pl.ANY)
    moved = 2 * num_rows + sum(caps) * shards
    return pl.pallas_call(
        functools.partial(apply_kernel, shards, caps, num_rows),
        out_shape=jax.ShapeDtypeStruct(table.shape, jnp.float32),
        in_specs=[pl.BlockSpec(memory_space=pltpu.SMEM)] * len(caps) + [pl.BlockSpec(memory_space=pltpu.VMEM), any_space] + [any_space] * len(caps),
        out_specs=any_space,
        scratch_shapes=[pltpu.VMEM((num_rows + TILE, depth), jnp.float32), pltpu.VMEM((BUFFERS, max(caps), depth), jnp.float32), pltpu.SemaphoreType.DMA, pltpu.SemaphoreType.DMA((BUFFERS,)), pltpu.SemaphoreType.DMA],
        compiler_params=pltpu.CompilerParams(vmem_limit_bytes=40 * 2**20),
        cost_estimate=pl.CostEstimate(flops=40 * moved * depth, bytes_accessed=4 * moved * depth, transcendentals=0),
        name='apply_rows',
    )(*rows, lent, table, *grads)


def solution(mesh):
    shards = mesh.shape[AXIS_NAME]

    def device_step(in_shard, out_shard, center_ids, context_ids, negative_ids):
        shard_rows, depth = in_shard.shape
        num_negs = negative_ids.shape[0]
        lists = (center_ids, context_ids, negative_ids)
        full = tuple(up8(distinct_bound(ids.shape[0], shards) + TILE) for ids in lists)
        usual = tuple(up8(TILE + ids.shape[0] * 13 // (16 * shards)) for ids in lists)

        owners, ranks, asks, largest = zip(*(request_layout(ids, shard_rows, shards, cap) for ids, cap in zip(lists, full)))
        counts = jnp.broadcast_to(jnp.stack(largest)[None, :], (shards, 3))
        ask = jnp.concatenate(asks + (counts,), axis=1)
        ask = jnp.pad(ask, ((0, 0), (0, HEADER * LANES - ask.shape[1]))).reshape(shards, HEADER, LANES)
        arrived, lent_in, lent_out = ask_owners(ask, in_shard, out_shard, shards)
        arrived = arrived.reshape(shards, HEADER * LANES)
        edge1, edge2, edge3 = full[0], full[0] + full[1], sum(full)
        slots = (arrived[:, :edge1], arrived[:, edge1:edge2], arrived[:, edge2:edge3])
        most = jnp.max(arrived[:, edge3:edge3 + 3], axis=0)
        unit = jnp.where(most[2] >= 0, 1.0, 0.0)
        fits = jnp.all(most <= jnp.array(usual, jnp.int32))

        def run(caps, in_shard, out_shard, lent_in, lent_out, owners, ranks, slots, unit):
            cell_of_id = [owner * cap + rank for owner, rank, cap in zip(owners, ranks, caps)]
            asked = [slot[:, :cap] for slot, cap in zip(slots, caps)]

            def pick(table, lent, slot):
                rows = take_rows(table, jnp.maximum(slot - TILE, 0))
                return lax.dynamic_update_slice(rows, jnp.broadcast_to(lent[None], (shards, TILE, depth)), (0, 0, 0))

            def fetch(rows):
                return exchange(rows).reshape(-1, depth)

            def send_back(grads, cells, cap):
                summed = jnp.zeros((shards * cap, depth), jnp.float32).at[cells].add(grads, mode='promise_in_bounds')
                return exchange(summed.reshape(shards, cap, depth))

            picked_neg, slot_in, slot_ctx = lax.optimization_barrier((pick(out_shard, lent_out, asked[2]), asked[0], asked[1]))
            neg_rows = fetch(picked_neg)
            picked_in, slot_ctx = lax.optimization_barrier((pick(in_shard, lent_in, slot_in), slot_ctx))
            in_rows = fetch(picked_in)
            ctx_rows = fetch(pick(out_shard, lent_out, slot_ctx))

            negative_half = (take_rows(neg_rows, cell_of_id[2]) * unit).astype(jnp.bfloat16)
            center_vec = take_rows(in_rows, cell_of_id[0])
            center_half = center_vec.astype(jnp.bfloat16)
            neg_score = dot_f32(center_half, negative_half, ((1,), (1,)))
            neg_grad = ((NEG_WEIGHT / num_negs) * jax.nn.sigmoid(neg_score)).astype(jnp.bfloat16)
            d_negative = -dot_f32(neg_grad, center_half, ((0,), (0,)))
            neg_back = send_back(d_negative, cell_of_id[2], caps[2])
            d_center_neg = dot_f32(neg_grad, negative_half, ((1,), (0,)))

            context_vec = take_rows(ctx_rows, cell_of_id[1])
            pos_grad = (jax.nn.sigmoid(jnp.sum(center_vec * context_vec, axis=1)) - 1.0)[:, None]
            ctx_back = send_back(-(pos_grad * center_vec), cell_of_id[1], caps[1])
            in_back = send_back(-(pos_grad * context_vec + d_center_neg), cell_of_id[0], caps[0])

            lent_sum = LEARN_RATE * (jnp.sum(neg_back[:, :TILE], axis=0) + jnp.sum(ctx_back[:, :TILE], axis=0))
            new_out = apply_rows(out_shard, collect_lent(lent_sum, shards), (asked[2], asked[1]), (neg_back, ctx_back))
            lent_sum = LEARN_RATE * jnp.sum(in_back[:, :TILE], axis=0)
            new_in = apply_rows(in_shard, collect_lent(lent_sum, shards), (asked[0],), (in_back,))
            return new_in, new_out

        def branch(caps):
            def call(*args):
                return run(caps, *args)

            return call

        args = (in_shard, out_shard, lent_in, lent_out, owners, ranks, slots, unit)
        return lax.cond(fits, branch(usual), branch(full), *args)

    return jax.shard_map(device_step, mesh=mesh, in_specs=(P(AXIS_NAME, None), P(AXIS_NAME, None), P(AXIS_NAME), P(AXIS_NAME), P(AXIS_NAME)), out_specs=(P(AXIS_NAME, None), P(AXIS_NAME, None)), check_vma=False)
```

```python
import functools

import jax
import jax.numpy as jnp
from jax import lax
from jax.experimental import pallas as pl
from jax.experimental.pallas import tpu as pltpu
from jax.sharding import PartitionSpec as P

LEARN_RATE = 1.0
NEG_WEIGHT = 5.0
AXIS_NAME = 'vp'
TILE = 8
LANES = 128
SLOT_BLOCKS = 16
HEADER = 8


def up8(count):
    return (count + 7) // 8 * 8


def distinct_bound(num_ids, shards):
    common_slots = 3 * num_ids // shards
    return common_slots // 4 + (num_ids - common_slots + shards - 1) // shards


def onehot(values, size):
    return (values[:, None] == lax.broadcasted_iota(jnp.int32, (1, size), 1)).astype(jnp.bfloat16)


def dot_f32(a, b, dims):
    return lax.dot_general(a, b, (dims, ((), ())), preferred_element_type=jnp.float32)


def request_layout(id_list, shard_rows, shards, capacity):
    hot = id_list < shards * TILE
    owner = jnp.where(hot, id_list // TILE, id_list // shard_rows)
    slot = jnp.where(hot, id_list % TILE, id_list % shard_rows + TILE)
    high = onehot(owner * SLOT_BLOCKS + slot // LANES, shards * SLOT_BLOCKS)
    low = onehot(slot % LANES, LANES)
    count = dot_f32(high, low, ((0,), (0,)))
    shape = (shards * SLOT_BLOCKS, LANES)
    row_idx = lax.broadcasted_iota(jnp.int32, shape, 0)
    lane_idx = lax.broadcasted_iota(jnp.int32, shape, 1)
    lent = (row_idx % SLOT_BLOCKS == 0) & (lane_idx < TILE)
    present = (count > 0.0) | lent
    ones = present.astype(jnp.bfloat16)
    upper = (lax.broadcasted_iota(jnp.int32, (LANES, LANES), 0) <= lax.broadcasted_iota(jnp.int32, (LANES, LANES), 1)).astype(jnp.bfloat16)
    inclusive = dot_f32(ones, upper, ((1,), (0,)))
    block_total = jnp.sum(present.astype(jnp.float32), axis=1).reshape(shards, SLOT_BLOCKS)
    before = (lax.broadcasted_iota(jnp.int32, (SLOT_BLOCKS, SLOT_BLOCKS), 0) < lax.broadcasted_iota(jnp.int32, (SLOT_BLOCKS, SLOT_BLOCKS), 1))
    block_start = dot_f32(block_total.astype(jnp.bfloat16), before.astype(jnp.bfloat16), ((1,), (0,)))
    rank = inclusive - ones.astype(jnp.float32) + block_start.reshape(-1)[:, None]
    largest = jnp.max(jnp.sum(block_total, axis=1)).astype(jnp.int32)
    rank_of_id = jnp.sum(dot_f32(high, rank.astype(jnp.bfloat16), ((1,), (0,))) * low.astype(jnp.float32), axis=1).astype(jnp.int32)
    rank_or_none = jnp.where(present, rank, -1.0).reshape(shards, 1, SLOT_BLOCKS * LANES)
    cells = lax.broadcasted_iota(jnp.int32, (1, capacity, 1), 1).astype(jnp.float32)
    slots = lax.broadcasted_iota(jnp.int32, (1, 1, SLOT_BLOCKS * LANES), 2).astype(jnp.float32)
    slot_of_cell = jnp.sum(jnp.where(rank_or_none == cells, slots + 1.0, 0.0), axis=2).astype(jnp.int32) - 1
    return owner, rank_of_id, slot_of_cell, largest


def exchange(blocks):
    return lax.all_to_all(blocks, AXIS_NAME, 0, 0)


def take_rows(rows, idx):
    return rows.at[idx].get(mode='promise_in_bounds')


def meet(me, shards):
    barrier = pltpu.get_barrier_semaphore()
    for step in range(1, shards):
        pl.semaphore_signal(barrier, inc=1, device_id=(lax.rem(me + step, shards),), device_id_type=pl.DeviceIdType.MESH)
    pl.semaphore_wait(barrier, shards - 1)


def remote(src, dst, send_sem, recv_sem, peer):
    return pltpu.make_async_remote_copy(src_ref=src, dst_ref=dst, send_sem=send_sem, recv_sem=recv_sem, device_id=(peer,), device_id_type=pl.DeviceIdType.MESH)


def ask_kernel(shards, ask, in_shard, out_shard, got, lent_in, lent_out, ask_send, ask_recv, lend_send, lend_recv, own_sem):
    me = lax.axis_index(AXIS_NAME)
    meet(me, shards)

    def lend(peer, part):
        table, lent = ((in_shard, lent_in), (out_shard, lent_out))[part]
        return remote(table.at[pl.ds(pl.multiple_of(peer * TILE, TILE), TILE)], lent, lend_send.at[part, peer], lend_recv.at[part], peer)

    @pl.when(me == 0)
    def _():
        for peer in range(1, shards):
            lend(peer, 0).start()
            lend(peer, 1).start()
        pltpu.make_async_copy(in_shard.at[pl.ds(0, TILE)], lent_in, own_sem.at[0]).start()
        pltpu.make_async_copy(out_shard.at[pl.ds(0, TILE)], lent_out, own_sem.at[1]).start()

    copies = []
    for step in range(1, shards):
        peer = lax.rem(me + step, shards)
        copies.append(remote(ask.at[peer], got.at[me], ask_send.at[step], ask_recv.at[step], peer))
        copies[-1].start()
    got[me] = ask[me]
    for copy in copies:
        copy.wait()

    @pl.when(me == 0)
    def _():
        for peer in range(1, shards):
            lend(peer, 0).wait_send()
            lend(peer, 1).wait_send()
        pltpu.make_async_copy(in_shard.at[pl.ds(0, TILE)], lent_in, own_sem.at[0]).wait()
        pltpu.make_async_copy(out_shard.at[pl.ds(0, TILE)], lent_out, own_sem.at[1]).wait()

    @pl.when(me != 0)
    def _():
        lend(me, 0).wait_recv()
        lend(me, 1).wait_recv()


def ask_owners(ask, in_shard, out_shard, shards):
    depth = in_shard.shape[1]
    any_space, vmem = pl.BlockSpec(memory_space=pl.ANY), pl.BlockSpec(memory_space=pltpu.VMEM)
    tile = jax.ShapeDtypeStruct((TILE, depth), jnp.float32)
    return pl.pallas_call(
        functools.partial(ask_kernel, shards),
        out_shape=(jax.ShapeDtypeStruct(ask.shape, jnp.int32), tile, tile),
        in_specs=[vmem, any_space, any_space],
        out_specs=(vmem, vmem, vmem),
        scratch_shapes=[pltpu.SemaphoreType.DMA((shards,)), pltpu.SemaphoreType.DMA((shards,)), pltpu.SemaphoreType.DMA((2, shards)), pltpu.SemaphoreType.DMA((2,)), pltpu.SemaphoreType.DMA((2,))],
        compiler_params=pltpu.CompilerParams(collective_id=0, has_side_effects=True),
        name='ask_owners',
    )(ask, in_shard, out_shard)


def exchange_kernel(shards, blocks, got, send_sem, recv_sem, own_sem):
    me = lax.axis_index(AXIS_NAME)
    meet(me, shards)
    own = pltpu.make_async_copy(blocks.at[me], got.at[me], own_sem)
    own.start()

    def copy(step, rows):
        peer = lax.rem(me + step, shards)
        return remote(blocks.at[peer, rows], got.at[me, rows], send_sem.at[step], recv_sem.at[step], peer)

    def send(tile, carry):
        for step in range(1, shards):
            copy(step, pl.ds(pl.multiple_of(tile * TILE, TILE), TILE)).start()
        return carry

    count = blocks.shape[1]
    lax.fori_loop(0, count // TILE, send, 0)
    for step in range(1, shards):
        copy(step, pl.ds(0, count)).wait()
    own.wait()


def exchange_rows(blocks, collective_id):
    shards = blocks.shape[0]
    any_space = pl.BlockSpec(memory_space=pl.ANY)
    return pl.pallas_call(
        functools.partial(exchange_kernel, shards),
        out_shape=jax.ShapeDtypeStruct(blocks.shape, jnp.float32),
        in_specs=[any_space],
        out_specs=any_space,
        scratch_shapes=[pltpu.SemaphoreType.DMA((shards,)), pltpu.SemaphoreType.DMA((shards,)), pltpu.SemaphoreType.DMA],
        compiler_params=pltpu.CompilerParams(collective_id=collective_id, has_side_effects=True),
    )(blocks)


def collect_kernel(shards, mine, got, send_sem, recv_sem):
    me = lax.axis_index(AXIS_NAME)
    ready = pltpu.get_barrier_semaphore()

    @pl.when(me == 0)
    def _():
        for peer in range(1, shards):
            pl.semaphore_signal(ready, inc=1, device_id=(peer,), device_id_type=pl.DeviceIdType.MESH)
        got[0] = mine[...]
        for peer in range(1, shards):
            remote(mine, got.at[peer], send_sem, recv_sem.at[peer], 0).wait_recv()

    @pl.when(me != 0)
    def _():
        pl.semaphore_wait(ready, 1)
        got[...] = jnp.zeros_like(got)
        copy = remote(mine, got.at[me], send_sem, recv_sem.at[me], 0)
        copy.start()
        copy.wait_send()


def collect_lent(mine, shards):
    vmem = pl.BlockSpec(memory_space=pltpu.VMEM)
    return pl.pallas_call(
        functools.partial(collect_kernel, shards),
        out_shape=jax.ShapeDtypeStruct((shards,) + mine.shape, jnp.float32),
        in_specs=[vmem],
        out_specs=vmem,
        scratch_shapes=[pltpu.SemaphoreType.DMA, pltpu.SemaphoreType.DMA((shards,))],
        compiler_params=pltpu.CompilerParams(collective_id=1, has_side_effects=True),
        name='collect_lent',
    )(mine)


GROUP = 4
BUFFERS = 4
PARTS = 2


def apply_kernel(shards, caps, num_rows, *refs):
    lists = len(caps)
    rows, (lent, table), grads, out = refs[:lists], refs[lists:lists + 2], refs[lists + 2:2 * lists + 2], refs[2 * lists + 2]
    total, buf, load_sem, grad_sem, store_sem = refs[2 * lists + 3:]
    width = table.shape[1] // PARTS
    segments = [(part, i) for part in range(PARTS) for i in range(lists)]

    def columns(part):
        return pl.ds(part * width, width)

    def load(part):
        return pltpu.make_async_copy(table.at[:, columns(part)], total.at[pl.ds(0, num_rows), columns(part)], load_sem.at[part])

    def store(part):
        return pltpu.make_async_copy(total.at[pl.ds(0, num_rows), columns(part)], out.at[:, columns(part)], store_sem.at[part])

    def copy(segment, source):
        part, i = segment
        place = lax.rem(source, BUFFERS)
        return pltpu.make_async_copy(grads[i].at[source, :, columns(part)], buf.at[place, pl.ds(0, caps[i])], grad_sem.at[place])

    for part in range(PARTS):
        load(part).start()
    for source in range(BUFFERS - 1):
        copy(segments[0], source).start()
    for number, segment in enumerate(segments):
        part, i = segment
        if i == 0:
            load(part).wait()
            total[pl.ds(0, lent.shape[0]), columns(part)] += lent[:, columns(part)]

        def from_source(source, carry):
            ahead = source + BUFFERS - 1

            @pl.when(ahead < shards)
            def _():
                copy(segment, ahead).start()

            if number + 1 < len(segments):
                @pl.when(ahead >= shards)
                def _():
                    copy(segments[number + 1], ahead - shards).start()

            copy(segment, source).wait()
            place = lax.rem(source, BUFFERS)

            def group(step, carry):
                base = source * caps[i] + step * GROUP
                idx = [rows[i][base + k] for k in range(GROUP)]
                sums = [total[pl.ds(idx[k], 1), columns(part)] + buf[place, pl.ds(step * GROUP + k, 1), :] for k in range(GROUP)]
                for k in range(GROUP):
                    total[pl.ds(idx[k], 1), columns(part)] = sums[k]
                return carry

            return lax.fori_loop(TILE // GROUP, caps[i] // GROUP, group, carry)

        lax.fori_loop(0, shards, from_source, 0)
        if i == lists - 1:
            store(part).start()
    for part in range(PARTS):
        store(part).wait()


def apply_rows(table, lent, slots, grads):
    num_rows, depth = table.shape
    shards = grads[0].shape[0]
    caps = tuple(g.shape[1] for g in grads)
    rows = [jnp.where(slot < TILE, num_rows, slot - TILE).reshape(-1) for slot in slots]
    any_space = pl.BlockSpec(memory_space=pl.ANY)
    moved = 2 * num_rows + sum(caps) * shards
    return pl.pallas_call(
        functools.partial(apply_kernel, shards, caps, num_rows),
        out_shape=jax.ShapeDtypeStruct(table.shape, jnp.float32),
        in_specs=[pl.BlockSpec(memory_space=pltpu.SMEM)] * len(caps) + [pl.BlockSpec(memory_space=pltpu.VMEM), any_space] + [any_space] * len(caps),
        out_specs=any_space,
        scratch_shapes=[pltpu.VMEM((num_rows + TILE, depth), jnp.float32), pltpu.VMEM((BUFFERS, max(caps), depth // PARTS), jnp.float32), pltpu.SemaphoreType.DMA((PARTS,)), pltpu.SemaphoreType.DMA((BUFFERS,)), pltpu.SemaphoreType.DMA((PARTS,))],
        compiler_params=pltpu.CompilerParams(vmem_limit_bytes=40 * 2**20),
        cost_estimate=pl.CostEstimate(flops=40 * moved * depth, bytes_accessed=4 * moved * depth, transcendentals=0),
        name='apply_rows',
    )(*rows, lent, table, *grads)


def solution(mesh):
    shards = mesh.shape[AXIS_NAME]

    def device_step(in_shard, out_shard, center_ids, context_ids, negative_ids):
        shard_rows, depth = in_shard.shape
        num_negs = negative_ids.shape[0]
        lists = (center_ids, context_ids, negative_ids)
        full = tuple(up8(distinct_bound(ids.shape[0], shards) + TILE) for ids in lists)
        usual = tuple(up8(TILE + ids.shape[0] * 13 // (16 * shards)) for ids in lists)

        owners, ranks, asks, largest = zip(*(request_layout(ids, shard_rows, shards, cap) for ids, cap in zip(lists, full)))
        counts = jnp.broadcast_to(jnp.stack(largest)[None, :], (shards, 3))
        ask = jnp.concatenate(asks + (counts,), axis=1)
        ask = jnp.pad(ask, ((0, 0), (0, HEADER * LANES - ask.shape[1]))).reshape(shards, HEADER, LANES)
        arrived, lent_in, lent_out = ask_owners(ask, in_shard, out_shard, shards)
        arrived = arrived.reshape(shards, HEADER * LANES)
        edge1, edge2, edge3 = full[0], full[0] + full[1], sum(full)
        slots = (arrived[:, :edge1], arrived[:, edge1:edge2], arrived[:, edge2:edge3])
        most = jnp.max(arrived[:, edge3:edge3 + 3], axis=0)
        unit = jnp.where(most[2] >= 0, 1.0, 0.0)
        fits = jnp.all(most <= jnp.array(usual, jnp.int32))

        def run(exchange, caps, in_shard, out_shard, lent_in, lent_out, owners, ranks, slots, unit):
            cell_of_id = [owner * cap + rank for owner, rank, cap in zip(owners, ranks, caps)]
            asked = [slot[:, :cap] for slot, cap in zip(slots, caps)]

            def pick(table, lent, slot):
                rows = take_rows(table, jnp.maximum(slot - TILE, 0))
                return lax.dynamic_update_slice(rows, jnp.broadcast_to(lent[None], (shards, TILE, depth)), (0, 0, 0))

            def fetch(rows):
                return exchange(rows).reshape(-1, depth)

            def send_back(grads, cells, cap):
                summed = jnp.zeros((shards * cap, depth), jnp.float32).at[cells].add(grads, mode='promise_in_bounds')
                return exchange(summed.reshape(shards, cap, depth))

            picked_neg, slot_in, slot_ctx = lax.optimization_barrier((pick(out_shard, lent_out, asked[2]), asked[0], asked[1]))
            neg_rows = fetch(picked_neg)
            picked_in, slot_ctx = lax.optimization_barrier((pick(in_shard, lent_in, slot_in), slot_ctx))
            in_rows = fetch(picked_in)
            ctx_rows = fetch(pick(out_shard, lent_out, slot_ctx))

            negative_half = (take_rows(neg_rows, cell_of_id[2]) * unit).astype(jnp.bfloat16)
            center_vec = take_rows(in_rows, cell_of_id[0])
            center_half = center_vec.astype(jnp.bfloat16)
            neg_score = dot_f32(center_half, negative_half, ((1,), (1,)))
            neg_grad = ((NEG_WEIGHT / num_negs) * jax.nn.sigmoid(neg_score)).astype(jnp.bfloat16)
            d_negative = -dot_f32(neg_grad, center_half, ((0,), (0,)))
            neg_back = send_back(d_negative, cell_of_id[2], caps[2])
            d_center_neg = dot_f32(neg_grad, negative_half, ((1,), (0,)))

            context_vec = take_rows(ctx_rows, cell_of_id[1])
            pos_grad = (jax.nn.sigmoid(jnp.sum(center_vec * context_vec, axis=1)) - 1.0)[:, None]
            ctx_back = send_back(-(pos_grad * center_vec), cell_of_id[1], caps[1])
            in_back = send_back(-(pos_grad * context_vec + d_center_neg), cell_of_id[0], caps[0])

            new_out = apply_rows(out_shard, jnp.zeros((TILE, depth), jnp.float32), (asked[2], asked[1]), (neg_back, ctx_back))
            sum_out = jnp.sum(neg_back[:, :TILE], axis=0) + jnp.sum(ctx_back[:, :TILE], axis=0)
            sum_in = jnp.sum(in_back[:, :TILE], axis=0)
            total = LEARN_RATE * collect_lent(jnp.concatenate([sum_in, sum_out], axis=0), shards)
            new_in = apply_rows(in_shard, total[:, :TILE].reshape(-1, depth), (asked[0],), (in_back,))
            new_out = new_out.at[:shards * TILE].add(total[:, TILE:].reshape(-1, depth))
            return new_in, new_out

        def exchange_full(blocks):
            return exchange_rows(blocks, 2 + (blocks.shape[1] == full[2]))

        def branch(swap, caps):
            def call(*args):
                return run(swap, caps, *args)

            return call

        args = (in_shard, out_shard, lent_in, lent_out, owners, ranks, slots, unit)
        return lax.cond(fits, branch(exchange, usual), branch(exchange_full, full), *args)

    return jax.shard_map(device_step, mesh=mesh, in_specs=(P(AXIS_NAME, None), P(AXIS_NAME, None), P(AXIS_NAME), P(AXIS_NAME), P(AXIS_NAME)), out_specs=(P(AXIS_NAME, None), P(AXIS_NAME, None)), check_vma=False)
```

```python
import functools

import jax
import jax.numpy as jnp
from jax import lax
from jax.experimental import pallas as pl
from jax.experimental.pallas import tpu as pltpu
from jax.sharding import PartitionSpec as P

LEARN_RATE = 1.0
NEG_WEIGHT = 5.0
AXIS_NAME = 'vp'
TILE = 8
LANES = 128
SLOT_BLOCKS = 16
HEADER = 8


def up8(count):
    return (count + 7) // 8 * 8


def distinct_bound(num_ids, shards):
    common_slots = 3 * num_ids // shards
    return common_slots // 4 + (num_ids - common_slots + shards - 1) // shards


def onehot(values, size):
    return (values[:, None] == lax.broadcasted_iota(jnp.int32, (1, size), 1)).astype(jnp.bfloat16)


def dot_f32(a, b, dims):
    return lax.dot_general(a, b, (dims, ((), ())), preferred_element_type=jnp.float32)


def request_layout(id_list, shard_rows, shards, capacity):
    hot = id_list < shards * TILE
    owner = jnp.where(hot, id_list // TILE, id_list // shard_rows)
    slot = jnp.where(hot, id_list % TILE, id_list % shard_rows + TILE)
    high = onehot(owner * SLOT_BLOCKS + slot // LANES, shards * SLOT_BLOCKS)
    low = onehot(slot % LANES, LANES)
    count = dot_f32(high, low, ((0,), (0,)))
    shape = (shards * SLOT_BLOCKS, LANES)
    row_idx = lax.broadcasted_iota(jnp.int32, shape, 0)
    lane_idx = lax.broadcasted_iota(jnp.int32, shape, 1)
    lent = (row_idx % SLOT_BLOCKS == 0) & (lane_idx < TILE)
    present = (count > 0.0) | lent
    ones = present.astype(jnp.bfloat16)
    upper = (lax.broadcasted_iota(jnp.int32, (LANES, LANES), 0) <= lax.broadcasted_iota(jnp.int32, (LANES, LANES), 1)).astype(jnp.bfloat16)
    inclusive = dot_f32(ones, upper, ((1,), (0,)))
    block_total = jnp.sum(present.astype(jnp.float32), axis=1).reshape(shards, SLOT_BLOCKS)
    before = (lax.broadcasted_iota(jnp.int32, (SLOT_BLOCKS, SLOT_BLOCKS), 0) < lax.broadcasted_iota(jnp.int32, (SLOT_BLOCKS, SLOT_BLOCKS), 1))
    block_start = dot_f32(block_total.astype(jnp.bfloat16), before.astype(jnp.bfloat16), ((1,), (0,)))
    rank = inclusive - ones.astype(jnp.float32) + block_start.reshape(-1)[:, None]
    largest = jnp.max(jnp.sum(block_total, axis=1)).astype(jnp.int32)
    rank_of_id = jnp.sum(dot_f32(high, rank.astype(jnp.bfloat16), ((1,), (0,))) * low.astype(jnp.float32), axis=1).astype(jnp.int32)
    rank_or_none = jnp.where(present, rank, -1.0).reshape(shards, 1, SLOT_BLOCKS * LANES)
    cells = lax.broadcasted_iota(jnp.int32, (1, capacity, 1), 1).astype(jnp.float32)
    slots = lax.broadcasted_iota(jnp.int32, (1, 1, SLOT_BLOCKS * LANES), 2).astype(jnp.float32)
    slot_of_cell = jnp.sum(jnp.where(rank_or_none == cells, slots + 1.0, 0.0), axis=2).astype(jnp.int32) - 1
    return owner, rank_of_id, slot_of_cell, largest


def exchange(blocks):
    return lax.all_to_all(blocks, AXIS_NAME, 0, 0)


def take_rows(rows, idx):
    return rows.at[idx].get(mode='promise_in_bounds')


def meet(me, shards):
    barrier = pltpu.get_barrier_semaphore()
    for step in range(1, shards):
        pl.semaphore_signal(barrier, inc=1, device_id=(lax.rem(me + step, shards),), device_id_type=pl.DeviceIdType.MESH)
    pl.semaphore_wait(barrier, shards - 1)


def remote(src, dst, send_sem, recv_sem, peer):
    return pltpu.make_async_remote_copy(src_ref=src, dst_ref=dst, send_sem=send_sem, recv_sem=recv_sem, device_id=(peer,), device_id_type=pl.DeviceIdType.MESH)


def ask_kernel(shards, ask, in_shard, out_shard, got, lent_in, lent_out, ask_send, ask_recv, lend_send, lend_recv, own_sem):
    me = lax.axis_index(AXIS_NAME)
    meet(me, shards)

    def lend(peer, part):
        table, lent = ((in_shard, lent_in), (out_shard, lent_out))[part]
        return remote(table.at[pl.ds(pl.multiple_of(peer * TILE, TILE), TILE)], lent, lend_send.at[part, peer], lend_recv.at[part], peer)

    @pl.when(me == 0)
    def _():
        for peer in range(1, shards):
            lend(peer, 0).start()
            lend(peer, 1).start()
        pltpu.make_async_copy(in_shard.at[pl.ds(0, TILE)], lent_in, own_sem.at[0]).start()
        pltpu.make_async_copy(out_shard.at[pl.ds(0, TILE)], lent_out, own_sem.at[1]).start()

    copies = []
    for step in range(1, shards):
        peer = lax.rem(me + step, shards)
        copies.append(remote(ask.at[peer], got.at[me], ask_send.at[step], ask_recv.at[step], peer))
        copies[-1].start()
    got[me] = ask[me]
    for copy in copies:
        copy.wait()

    @pl.when(me == 0)
    def _():
        for peer in range(1, shards):
            lend(peer, 0).wait_send()
            lend(peer, 1).wait_send()
        pltpu.make_async_copy(in_shard.at[pl.ds(0, TILE)], lent_in, own_sem.at[0]).wait()
        pltpu.make_async_copy(out_shard.at[pl.ds(0, TILE)], lent_out, own_sem.at[1]).wait()

    @pl.when(me != 0)
    def _():
        lend(me, 0).wait_recv()
        lend(me, 1).wait_recv()


def ask_owners(ask, in_shard, out_shard, shards):
    depth = in_shard.shape[1]
    any_space, vmem = pl.BlockSpec(memory_space=pl.ANY), pl.BlockSpec(memory_space=pltpu.VMEM)
    tile = jax.ShapeDtypeStruct((TILE, depth), jnp.float32)
    return pl.pallas_call(
        functools.partial(ask_kernel, shards),
        out_shape=(jax.ShapeDtypeStruct(ask.shape, jnp.int32), tile, tile),
        in_specs=[vmem, any_space, any_space],
        out_specs=(vmem, vmem, vmem),
        scratch_shapes=[pltpu.SemaphoreType.DMA((shards,)), pltpu.SemaphoreType.DMA((shards,)), pltpu.SemaphoreType.DMA((2, shards)), pltpu.SemaphoreType.DMA((2,)), pltpu.SemaphoreType.DMA((2,))],
        compiler_params=pltpu.CompilerParams(collective_id=0, has_side_effects=True),
        name='ask_owners',
    )(ask, in_shard, out_shard)


def exchange_kernel(shards, blocks, got, send_sem, recv_sem, own_sem):
    me = lax.axis_index(AXIS_NAME)
    meet(me, shards)
    own = pltpu.make_async_copy(blocks.at[me], got.at[me], own_sem)
    own.start()

    def copy(step, rows):
        peer = lax.rem(me + step, shards)
        return remote(blocks.at[peer, rows], got.at[me, rows], send_sem.at[step], recv_sem.at[step], peer)

    def send(tile, carry):
        for step in range(1, shards):
            copy(step, pl.ds(pl.multiple_of(tile * TILE, TILE), TILE)).start()
        return carry

    count = blocks.shape[1]
    lax.fori_loop(0, count // TILE, send, 0)
    for step in range(1, shards):
        copy(step, pl.ds(0, count)).wait()
    own.wait()


def exchange_rows(blocks, collective_id):
    shards = blocks.shape[0]
    any_space = pl.BlockSpec(memory_space=pl.ANY)
    return pl.pallas_call(
        functools.partial(exchange_kernel, shards),
        out_shape=jax.ShapeDtypeStruct(blocks.shape, jnp.float32),
        in_specs=[any_space],
        out_specs=any_space,
        scratch_shapes=[pltpu.SemaphoreType.DMA((shards,)), pltpu.SemaphoreType.DMA((shards,)), pltpu.SemaphoreType.DMA],
        compiler_params=pltpu.CompilerParams(collective_id=collective_id, has_side_effects=True),
    )(blocks)


def fetch_kernel(shards, in_idx, ctx_idx, neg_blocks, in_shard, out_shard, lent_in, lent_out, neg_got, in_got, in_blocks, ctx_blocks,
                 held, stage, neg_send, neg_recv, in_send, in_recv, own_sem, load_sem, stage_sem):
    me = lax.axis_index(AXIS_NAME)
    load_in = pltpu.make_async_copy(in_shard, held, load_sem)
    load_in.start()
    meet(me, shards)

    def exchange(blocks, got, send_sem, recv_sem):
        count = blocks.shape[1]

        def copy(step, rows):
            peer = lax.rem(me + step, shards)
            return remote(blocks.at[peer, rows], got.at[me, rows], send_sem.at[step], recv_sem.at[step], peer)

        def send(tile, carry):
            for step in range(1, shards):
                copy(step, pl.ds(pl.multiple_of(tile * TILE, TILE), TILE)).start()
            return carry

        def finish():
            for step in range(1, shards):
                copy(step, pl.ds(0, count)).wait()

        lax.fori_loop(0, count // TILE, send, 0)
        return finish

    def pick(idx, lent, blocks):
        count = blocks.shape[1]

        def put(peer, place):
            return pltpu.make_async_copy(stage.at[place, pl.ds(0, count)], blocks.at[peer], stage_sem.at[place])

        def for_peer(peer, carry):
            place = lax.rem(peer, 2)

            @pl.when(peer >= 2)
            def _():
                put(peer - 2, place).wait()

            stage[place, pl.ds(0, TILE), :] = lent[...]

            def group(step, carry):
                first = step * TILE
                for k in range(TILE):
                    stage[place, pl.ds(first + k, 1), :] = held[pl.ds(idx[peer * count + first + k], 1), :]
                return carry

            lax.fori_loop(1, count // TILE, group, 0)
            put(peer, place).start()
            return carry

        lax.fori_loop(0, shards, for_peer, 0)
        put(shards - 2, 0).wait()
        put(shards - 1, 1).wait()

    finish_neg = exchange(neg_blocks, neg_got, neg_send, neg_recv)
    own_neg = pltpu.make_async_copy(neg_blocks.at[me], neg_got.at[me], own_sem.at[0])
    own_neg.start()
    load_in.wait()
    pick(in_idx, lent_in, in_blocks)
    finish_in = exchange(in_blocks, in_got, in_send, in_recv)
    own_in = pltpu.make_async_copy(in_blocks.at[me], in_got.at[me], own_sem.at[1])
    own_in.start()
    load_out = pltpu.make_async_copy(out_shard, held, load_sem)
    load_out.start()
    load_out.wait()
    pick(ctx_idx, lent_out, ctx_blocks)
    own_neg.wait()
    own_in.wait()
    finish_neg()
    finish_in()


def fetch_rows(in_slot, ctx_slot, neg_blocks, in_shard, out_shard, lent_in, lent_out, collective_id):
    shards, in_cap = in_slot.shape
    ctx_cap, depth = ctx_slot.shape[1], in_shard.shape[1]
    smem, vmem, any_space = (pl.BlockSpec(memory_space=space) for space in (pltpu.SMEM, pltpu.VMEM, pl.ANY))
    in_shape = jax.ShapeDtypeStruct((shards, in_cap, depth), jnp.float32)
    ctx_shape = jax.ShapeDtypeStruct((shards, ctx_cap, depth), jnp.float32)
    sems = pltpu.SemaphoreType.DMA((shards,))
    neg_got, in_got, _, ctx_blocks = pl.pallas_call(
        functools.partial(fetch_kernel, shards),
        out_shape=(jax.ShapeDtypeStruct(neg_blocks.shape, jnp.float32), in_shape, in_shape, ctx_shape),
        in_specs=[smem, smem, any_space, any_space, any_space, vmem, vmem],
        out_specs=(any_space,) * 4,
        scratch_shapes=[pltpu.VMEM(in_shard.shape, jnp.float32), pltpu.VMEM((2, max(in_cap, ctx_cap), depth), jnp.float32), sems, sems, sems, sems, pltpu.SemaphoreType.DMA((2,)), pltpu.SemaphoreType.DMA, pltpu.SemaphoreType.DMA((2,))],
        compiler_params=pltpu.CompilerParams(collective_id=collective_id, has_side_effects=True, vmem_limit_bytes=40 * 2**20),
    )(jnp.maximum(in_slot - TILE, 0).reshape(-1), jnp.maximum(ctx_slot - TILE, 0).reshape(-1), neg_blocks, in_shard, out_shard, lent_in, lent_out)
    return neg_got.reshape(-1, depth), in_got.reshape(-1, depth), ctx_blocks


def collect_kernel(shards, mine, got, send_sem, recv_sem):
    me = lax.axis_index(AXIS_NAME)
    ready = pltpu.get_barrier_semaphore()

    @pl.when(me == 0)
    def _():
        for peer in range(1, shards):
            pl.semaphore_signal(ready, inc=1, device_id=(peer,), device_id_type=pl.DeviceIdType.MESH)
        got[0] = mine[...]
        for peer in range(1, shards):
            remote(mine, got.at[peer], send_sem, recv_sem.at[peer], 0).wait_recv()

    @pl.when(me != 0)
    def _():
        pl.semaphore_wait(ready, 1)
        got[...] = jnp.zeros_like(got)
        copy = remote(mine, got.at[me], send_sem, recv_sem.at[me], 0)
        copy.start()
        copy.wait_send()


def collect_lent(mine, shards):
    vmem = pl.BlockSpec(memory_space=pltpu.VMEM)
    return pl.pallas_call(
        functools.partial(collect_kernel, shards),
        out_shape=jax.ShapeDtypeStruct((shards,) + mine.shape, jnp.float32),
        in_specs=[vmem],
        out_specs=vmem,
        scratch_shapes=[pltpu.SemaphoreType.DMA, pltpu.SemaphoreType.DMA((shards,))],
        compiler_params=pltpu.CompilerParams(collective_id=1, has_side_effects=True),
        name='collect_lent',
    )(mine)


GROUP = 4
BUFFERS = 4
PARTS = 2


def apply_kernel(shards, caps, num_rows, *refs):
    lists = len(caps)
    rows, (lent, table), grads, out = refs[:lists], refs[lists:lists + 2], refs[lists + 2:2 * lists + 2], refs[2 * lists + 2]
    total, buf, load_sem, grad_sem, store_sem = refs[2 * lists + 3:]
    width = table.shape[1] // PARTS
    segments = [(part, i) for part in range(PARTS) for i in range(lists)]

    def columns(part):
        return pl.ds(part * width, width)

    def load(part):
        return pltpu.make_async_copy(table.at[:, columns(part)], total.at[pl.ds(0, num_rows), columns(part)], load_sem.at[part])

    def store(part):
        return pltpu.make_async_copy(total.at[pl.ds(0, num_rows), columns(part)], out.at[:, columns(part)], store_sem.at[part])

    def copy(segment, source):
        part, i = segment
        place = lax.rem(source, BUFFERS)
        return pltpu.make_async_copy(grads[i].at[source, :, columns(part)], buf.at[place, pl.ds(0, caps[i])], grad_sem.at[place])

    for part in range(PARTS):
        load(part).start()
    for source in range(BUFFERS - 1):
        copy(segments[0], source).start()
    for number, segment in enumerate(segments):
        part, i = segment
        if i == 0:
            load(part).wait()
            total[pl.ds(0, lent.shape[0]), columns(part)] += lent[:, columns(part)]

        def from_source(source, carry):
            ahead = source + BUFFERS - 1

            @pl.when(ahead < shards)
            def _():
                copy(segment, ahead).start()

            if number + 1 < len(segments):
                @pl.when(ahead >= shards)
                def _():
                    copy(segments[number + 1], ahead - shards).start()

            copy(segment, source).wait()
            place = lax.rem(source, BUFFERS)

            def group(step, carry):
                base = source * caps[i] + step * GROUP
                idx = [rows[i][base + k] for k in range(GROUP)]
                sums = [total[pl.ds(idx[k], 1), columns(part)] + buf[place, pl.ds(step * GROUP + k, 1), :] for k in range(GROUP)]
                for k in range(GROUP):
                    total[pl.ds(idx[k], 1), columns(part)] = sums[k]
                return carry

            return lax.fori_loop(TILE // GROUP, caps[i] // GROUP, group, carry)

        lax.fori_loop(0, shards, from_source, 0)
        if i == lists - 1:
            store(part).start()
    for part in range(PARTS):
        store(part).wait()


def apply_rows(table, lent, slots, grads):
    num_rows, depth = table.shape
    shards = grads[0].shape[0]
    caps = tuple(g.shape[1] for g in grads)
    rows = [jnp.where(slot < TILE, num_rows, slot - TILE).reshape(-1) for slot in slots]
    any_space = pl.BlockSpec(memory_space=pl.ANY)
    moved = 2 * num_rows + sum(caps) * shards
    return pl.pallas_call(
        functools.partial(apply_kernel, shards, caps, num_rows),
        out_shape=jax.ShapeDtypeStruct(table.shape, jnp.float32),
        in_specs=[pl.BlockSpec(memory_space=pltpu.SMEM)] * len(caps) + [pl.BlockSpec(memory_space=pltpu.VMEM), any_space] + [any_space] * len(caps),
        out_specs=any_space,
        scratch_shapes=[pltpu.VMEM((num_rows + TILE, depth), jnp.float32), pltpu.VMEM((BUFFERS, max(caps), depth // PARTS), jnp.float32), pltpu.SemaphoreType.DMA((PARTS,)), pltpu.SemaphoreType.DMA((BUFFERS,)), pltpu.SemaphoreType.DMA((PARTS,))],
        compiler_params=pltpu.CompilerParams(vmem_limit_bytes=40 * 2**20),
        cost_estimate=pl.CostEstimate(flops=40 * moved * depth, bytes_accessed=4 * moved * depth, transcendentals=0),
        name='apply_rows',
    )(*rows, lent, table, *grads)


def solution(mesh):
    shards = mesh.shape[AXIS_NAME]

    def device_step(in_shard, out_shard, center_ids, context_ids, negative_ids):
        shard_rows, depth = in_shard.shape
        num_negs = negative_ids.shape[0]
        lists = (center_ids, context_ids, negative_ids)
        full = tuple(up8(distinct_bound(ids.shape[0], shards) + TILE) for ids in lists)
        usual = tuple(up8(TILE + ids.shape[0] * 13 // (16 * shards)) for ids in lists)

        owners, ranks, asks, largest = zip(*(request_layout(ids, shard_rows, shards, cap) for ids, cap in zip(lists, full)))
        counts = jnp.broadcast_to(jnp.stack(largest)[None, :], (shards, 3))
        ask = jnp.concatenate(asks + (counts,), axis=1)
        ask = jnp.pad(ask, ((0, 0), (0, HEADER * LANES - ask.shape[1]))).reshape(shards, HEADER, LANES)
        arrived, lent_in, lent_out = ask_owners(ask, in_shard, out_shard, shards)
        arrived = arrived.reshape(shards, HEADER * LANES)
        edge1, edge2, edge3 = full[0], full[0] + full[1], sum(full)
        slots = (arrived[:, :edge1], arrived[:, edge1:edge2], arrived[:, edge2:edge3])
        most = jnp.max(arrived[:, edge3:edge3 + 3], axis=0)
        fits = jnp.all(most <= jnp.array(usual, jnp.int32))

        def run(exchange, caps, in_shard, out_shard, lent_in, lent_out, owners, ranks, slots):
            cell_of_id = [owner * cap + rank for owner, rank, cap in zip(owners, ranks, caps)]
            asked = [slot[:, :cap] for slot, cap in zip(slots, caps)]

            def pick(table, lent, slot):
                rows = take_rows(table, jnp.maximum(slot - TILE, 0))
                return lax.dynamic_update_slice(rows, jnp.broadcast_to(lent[None], (shards, TILE, depth)), (0, 0, 0))

            def send_back(grads, cells, cap):
                summed = jnp.zeros((shards * cap, depth), jnp.float32).at[cells].add(grads, mode='promise_in_bounds')
                return exchange(summed.reshape(shards, cap, depth))

            picked = pick(out_shard, lent_out, asked[2])
            neg_rows, in_rows, ctx_blocks = fetch_rows(asked[0], asked[1], picked, in_shard, out_shard, lent_in, lent_out, 4 if caps == usual else 5)
            ctx_rows = exchange(ctx_blocks).reshape(-1, depth)

            negative_half = take_rows(neg_rows, cell_of_id[2]).astype(jnp.bfloat16)
            center_vec = take_rows(in_rows, cell_of_id[0])
            center_half = center_vec.astype(jnp.bfloat16)
            neg_score = dot_f32(center_half, negative_half, ((1,), (1,)))
            neg_grad = ((NEG_WEIGHT / num_negs) * jax.nn.sigmoid(neg_score)).astype(jnp.bfloat16)
            d_negative = -dot_f32(neg_grad, center_half, ((0,), (0,)))
            neg_back = send_back(d_negative, cell_of_id[2], caps[2])
            d_center_neg = dot_f32(neg_grad, negative_half, ((1,), (0,)))

            context_vec = take_rows(ctx_rows, cell_of_id[1])
            pos_grad = (jax.nn.sigmoid(jnp.sum(center_vec * context_vec, axis=1)) - 1.0)[:, None]
            ctx_back = send_back(-(pos_grad * center_vec), cell_of_id[1], caps[1])
            in_back = send_back(-(pos_grad * context_vec + d_center_neg), cell_of_id[0], caps[0])

            new_out = apply_rows(out_shard, jnp.zeros((TILE, depth), jnp.float32), (asked[2], asked[1]), (neg_back, ctx_back))
            sum_out = jnp.sum(neg_back[:, :TILE], axis=0) + jnp.sum(ctx_back[:, :TILE], axis=0)
            sum_in = jnp.sum(in_back[:, :TILE], axis=0)
            total = LEARN_RATE * collect_lent(jnp.concatenate([sum_in, sum_out], axis=0), shards)
            new_in = apply_rows(in_shard, total[:, :TILE].reshape(-1, depth), (asked[0],), (in_back,))
            new_out = new_out.at[:shards * TILE].add(total[:, TILE:].reshape(-1, depth))
            return new_in, new_out

        def exchange_full(blocks):
            return exchange_rows(blocks, 2 + (blocks.shape[1] == full[2]))

        def branch(swap, caps):
            def call(*args):
                return run(swap, caps, *args)

            return call

        args = (in_shard, out_shard, lent_in, lent_out, owners, ranks, slots)
        return lax.cond(fits, branch(exchange, usual), branch(exchange_full, full), *args)

    return jax.shard_map(device_step, mesh=mesh, in_specs=(P(AXIS_NAME, None), P(AXIS_NAME, None), P(AXIS_NAME), P(AXIS_NAME), P(AXIS_NAME)), out_specs=(P(AXIS_NAME, None), P(AXIS_NAME, None)), check_vma=False)
```

```python
import functools

import jax
import jax.numpy as jnp
from jax import lax
from jax.experimental import pallas as pl
from jax.experimental.pallas import tpu as pltpu
from jax.sharding import PartitionSpec as P

LEARN_RATE = 1.0
NEG_WEIGHT = 5.0
AXIS_NAME = 'vp'
TILE = 8
LANES = 128
SLOT_BLOCKS = 16
HEADER = 8


def up8(count):
    return (count + 7) // 8 * 8


def distinct_bound(num_ids, shards):
    common_slots = 3 * num_ids // shards
    return common_slots // 4 + (num_ids - common_slots + shards - 1) // shards


def onehot(values, size):
    return (values[:, None] == lax.broadcasted_iota(jnp.int32, (1, size), 1)).astype(jnp.bfloat16)


def dot_f32(a, b, dims):
    return lax.dot_general(a, b, (dims, ((), ())), preferred_element_type=jnp.float32)


def request_layout(id_list, shard_rows, shards, capacity):
    hot = id_list < shards * TILE
    owner = jnp.where(hot, id_list // TILE, id_list // shard_rows)
    slot = jnp.where(hot, id_list % TILE, id_list % shard_rows + TILE)
    high = onehot(owner * SLOT_BLOCKS + slot // LANES, shards * SLOT_BLOCKS)
    low = onehot(slot % LANES, LANES)
    count = dot_f32(high, low, ((0,), (0,)))
    shape = (shards * SLOT_BLOCKS, LANES)
    row_idx = lax.broadcasted_iota(jnp.int32, shape, 0)
    lane_idx = lax.broadcasted_iota(jnp.int32, shape, 1)
    lent = (row_idx % SLOT_BLOCKS == 0) & (lane_idx < TILE)
    present = (count > 0.0) | lent
    ones = present.astype(jnp.bfloat16)
    upper = (lax.broadcasted_iota(jnp.int32, (LANES, LANES), 0) <= lax.broadcasted_iota(jnp.int32, (LANES, LANES), 1)).astype(jnp.bfloat16)
    inclusive = dot_f32(ones, upper, ((1,), (0,)))
    block_total = jnp.sum(present.astype(jnp.float32), axis=1).reshape(shards, SLOT_BLOCKS)
    before = (lax.broadcasted_iota(jnp.int32, (SLOT_BLOCKS, SLOT_BLOCKS), 0) < lax.broadcasted_iota(jnp.int32, (SLOT_BLOCKS, SLOT_BLOCKS), 1))
    block_start = dot_f32(block_total.astype(jnp.bfloat16), before.astype(jnp.bfloat16), ((1,), (0,)))
    rank = inclusive - ones.astype(jnp.float32) + block_start.reshape(-1)[:, None]
    largest = jnp.max(jnp.sum(block_total, axis=1)).astype(jnp.int32)
    rank_of_id = jnp.sum(dot_f32(high, rank.astype(jnp.bfloat16), ((1,), (0,))) * low.astype(jnp.float32), axis=1).astype(jnp.int32)
    rank_or_none = jnp.where(present, rank, -1.0).reshape(shards, 1, SLOT_BLOCKS * LANES)
    cells = lax.broadcasted_iota(jnp.int32, (1, capacity, 1), 1).astype(jnp.float32)
    slots = lax.broadcasted_iota(jnp.int32, (1, 1, SLOT_BLOCKS * LANES), 2).astype(jnp.float32)
    slot_of_cell = jnp.sum(jnp.where(rank_or_none == cells, slots + 1.0, 0.0), axis=2).astype(jnp.int32) - 1
    return owner, rank_of_id, slot_of_cell, largest


def exchange(blocks):
    return lax.all_to_all(blocks, AXIS_NAME, 0, 0)


def take_rows(rows, idx):
    return rows.at[idx].get(mode='promise_in_bounds')


def meet(me, shards):
    barrier = pltpu.get_barrier_semaphore()
    for step in range(1, shards):
        pl.semaphore_signal(barrier, inc=1, device_id=(lax.rem(me + step, shards),), device_id_type=pl.DeviceIdType.MESH)
    pl.semaphore_wait(barrier, shards - 1)


def remote(src, dst, send_sem, recv_sem, peer):
    return pltpu.make_async_remote_copy(src_ref=src, dst_ref=dst, send_sem=send_sem, recv_sem=recv_sem, device_id=(peer,), device_id_type=pl.DeviceIdType.MESH)


def ask_kernel(shards, ask, in_shard, out_shard, got, lent_in, lent_out, ask_send, ask_recv, lend_send, lend_recv, own_sem):
    me = lax.axis_index(AXIS_NAME)
    meet(me, shards)

    def lend(peer, part):
        table, lent = ((in_shard, lent_in), (out_shard, lent_out))[part]
        return remote(table.at[pl.ds(pl.multiple_of(peer * TILE, TILE), TILE)], lent, lend_send.at[part, peer], lend_recv.at[part], peer)

    @pl.when(me == 0)
    def _():
        for peer in range(1, shards):
            lend(peer, 0).start()
            lend(peer, 1).start()
        pltpu.make_async_copy(in_shard.at[pl.ds(0, TILE)], lent_in, own_sem.at[0]).start()
        pltpu.make_async_copy(out_shard.at[pl.ds(0, TILE)], lent_out, own_sem.at[1]).start()

    copies = []
    for step in range(1, shards):
        peer = lax.rem(me + step, shards)
        copies.append(remote(ask.at[peer], got.at[me], ask_send.at[step], ask_recv.at[step], peer))
        copies[-1].start()
    got[me] = ask[me]
    for copy in copies:
        copy.wait()

    @pl.when(me == 0)
    def _():
        for peer in range(1, shards):
            lend(peer, 0).wait_send()
            lend(peer, 1).wait_send()
        pltpu.make_async_copy(in_shard.at[pl.ds(0, TILE)], lent_in, own_sem.at[0]).wait()
        pltpu.make_async_copy(out_shard.at[pl.ds(0, TILE)], lent_out, own_sem.at[1]).wait()

    @pl.when(me != 0)
    def _():
        lend(me, 0).wait_recv()
        lend(me, 1).wait_recv()


def ask_owners(ask, in_shard, out_shard, shards):
    depth = in_shard.shape[1]
    any_space, vmem = pl.BlockSpec(memory_space=pl.ANY), pl.BlockSpec(memory_space=pltpu.VMEM)
    tile = jax.ShapeDtypeStruct((TILE, depth), jnp.float32)
    return pl.pallas_call(
        functools.partial(ask_kernel, shards),
        out_shape=(jax.ShapeDtypeStruct(ask.shape, jnp.int32), tile, tile),
        in_specs=[vmem, any_space, any_space],
        out_specs=(vmem, vmem, vmem),
        scratch_shapes=[pltpu.SemaphoreType.DMA((shards,)), pltpu.SemaphoreType.DMA((shards,)), pltpu.SemaphoreType.DMA((2, shards)), pltpu.SemaphoreType.DMA((2,)), pltpu.SemaphoreType.DMA((2,))],
        compiler_params=pltpu.CompilerParams(collective_id=0, has_side_effects=True),
        name='ask_owners',
    )(ask, in_shard, out_shard)


def exchange_kernel(shards, blocks, got, send_sem, recv_sem, own_sem):
    me = lax.axis_index(AXIS_NAME)
    meet(me, shards)
    own = pltpu.make_async_copy(blocks.at[me], got.at[me], own_sem)
    own.start()

    def copy(step, rows):
        peer = lax.rem(me + step, shards)
        return remote(blocks.at[peer, rows], got.at[me, rows], send_sem.at[step], recv_sem.at[step], peer)

    def send(tile, carry):
        for step in range(1, shards):
            copy(step, pl.ds(pl.multiple_of(tile * TILE, TILE), TILE)).start()
        return carry

    count = blocks.shape[1]
    lax.fori_loop(0, count // TILE, send, 0)
    for step in range(1, shards):
        copy(step, pl.ds(0, count)).wait()
    own.wait()


def exchange_rows(blocks, collective_id):
    shards = blocks.shape[0]
    any_space = pl.BlockSpec(memory_space=pl.ANY)
    return pl.pallas_call(
        functools.partial(exchange_kernel, shards),
        out_shape=jax.ShapeDtypeStruct(blocks.shape, jnp.float32),
        in_specs=[any_space],
        out_specs=any_space,
        scratch_shapes=[pltpu.SemaphoreType.DMA((shards,)), pltpu.SemaphoreType.DMA((shards,)), pltpu.SemaphoreType.DMA],
        compiler_params=pltpu.CompilerParams(collective_id=collective_id, has_side_effects=True),
    )(blocks)


def fetch_kernel(shards, in_idx, ctx_idx, neg_blocks, in_shard, out_shard, lent_in, neg_got, in_got, in_blocks, ctx_blocks,
                 held, stage, neg_send, neg_recv, in_send, in_recv, own_sem, load_sem, stage_sem):
    me = lax.axis_index(AXIS_NAME)
    load_in = pltpu.make_async_copy(in_shard, held, load_sem)
    load_in.start()
    meet(me, shards)

    def exchange(blocks, got, send_sem, recv_sem):
        count = blocks.shape[1]

        def copy(step, rows):
            peer = lax.rem(me + step, shards)
            return remote(blocks.at[peer, rows], got.at[me, rows], send_sem.at[step], recv_sem.at[step], peer)

        def send(tile, carry):
            for step in range(1, shards):
                copy(step, pl.ds(pl.multiple_of(tile * TILE, TILE), TILE)).start()
            return carry

        def finish():
            for step in range(1, shards):
                copy(step, pl.ds(0, count)).wait()

        lax.fori_loop(0, count // TILE, send, 0)
        return finish

    def pick(idx, lent, blocks):
        count = blocks.shape[1]

        def put(peer, place):
            return pltpu.make_async_copy(stage.at[place, pl.ds(0, count)], blocks.at[peer], stage_sem.at[place])

        def for_peer(peer, carry):
            place = lax.rem(peer, 2)

            @pl.when(peer >= 2)
            def _():
                put(peer - 2, place).wait()

            if lent is not None:
                stage[place, pl.ds(0, TILE), :] = lent[...]

            def group(step, carry):
                first = step * TILE
                for k in range(TILE):
                    stage[place, pl.ds(first + k, 1), :] = held[pl.ds(idx[peer * count + first + k], 1), :]
                return carry

            lax.fori_loop(0 if lent is None else 1, count // TILE, group, 0)
            put(peer, place).start()
            return carry

        lax.fori_loop(0, shards, for_peer, 0)
        put(shards - 2, 0).wait()
        put(shards - 1, 1).wait()

    finish_neg = exchange(neg_blocks, neg_got, neg_send, neg_recv)
    own_neg = pltpu.make_async_copy(neg_blocks.at[me], neg_got.at[me], own_sem.at[0])
    own_neg.start()
    load_in.wait()
    pick(in_idx, lent_in, in_blocks)
    finish_in = exchange(in_blocks, in_got, in_send, in_recv)
    own_in = pltpu.make_async_copy(in_blocks.at[me], in_got.at[me], own_sem.at[1])
    own_in.start()
    load_out = pltpu.make_async_copy(out_shard, held, load_sem)
    load_out.start()
    load_out.wait()
    pick(ctx_idx, None, ctx_blocks)
    own_neg.wait()
    own_in.wait()
    finish_neg()
    finish_in()


def fetch_rows(in_slot, ctx_slot, neg_blocks, in_shard, out_shard, lent_in, collective_id):
    shards, in_cap = in_slot.shape
    ctx_cap, depth = ctx_slot.shape[1], in_shard.shape[1]
    smem, vmem, any_space = (pl.BlockSpec(memory_space=space) for space in (pltpu.SMEM, pltpu.VMEM, pl.ANY))
    in_shape = jax.ShapeDtypeStruct((shards, in_cap, depth), jnp.float32)
    ctx_shape = jax.ShapeDtypeStruct((shards, ctx_cap, depth), jnp.float32)
    sems = pltpu.SemaphoreType.DMA((shards,))
    neg_got, in_got, _, ctx_blocks = pl.pallas_call(
        functools.partial(fetch_kernel, shards),
        out_shape=(jax.ShapeDtypeStruct(neg_blocks.shape, jnp.float32), in_shape, in_shape, ctx_shape),
        in_specs=[smem, smem, any_space, any_space, any_space, vmem],
        out_specs=(any_space,) * 4,
        scratch_shapes=[pltpu.VMEM(in_shard.shape, jnp.float32), pltpu.VMEM((2, max(in_cap, ctx_cap), depth), jnp.float32), sems, sems, sems, sems, pltpu.SemaphoreType.DMA((2,)), pltpu.SemaphoreType.DMA, pltpu.SemaphoreType.DMA((2,))],
        compiler_params=pltpu.CompilerParams(collective_id=collective_id, has_side_effects=True, vmem_limit_bytes=40 * 2**20),
    )(jnp.maximum(in_slot - TILE, 0).reshape(-1), jnp.maximum(ctx_slot - TILE, 0).reshape(-1), neg_blocks, in_shard, out_shard, lent_in)
    return neg_got.reshape(-1, depth), in_got.reshape(-1, depth), ctx_blocks


def collect_kernel(shards, mine, got, send_sem, recv_sem):
    me = lax.axis_index(AXIS_NAME)
    ready = pltpu.get_barrier_semaphore()

    @pl.when(me == 0)
    def _():
        for peer in range(1, shards):
            pl.semaphore_signal(ready, inc=1, device_id=(peer,), device_id_type=pl.DeviceIdType.MESH)
        got[0] = mine[...]
        for peer in range(1, shards):
            remote(mine, got.at[peer], send_sem, recv_sem.at[peer], 0).wait_recv()

    @pl.when(me != 0)
    def _():
        pl.semaphore_wait(ready, 1)
        got[...] = jnp.zeros_like(got)
        copy = remote(mine, got.at[me], send_sem, recv_sem.at[me], 0)
        copy.start()
        copy.wait_send()


def collect_lent(mine, shards):
    vmem = pl.BlockSpec(memory_space=pltpu.VMEM)
    return pl.pallas_call(
        functools.partial(collect_kernel, shards),
        out_shape=jax.ShapeDtypeStruct((shards,) + mine.shape, jnp.float32),
        in_specs=[vmem],
        out_specs=vmem,
        scratch_shapes=[pltpu.SemaphoreType.DMA, pltpu.SemaphoreType.DMA((shards,))],
        compiler_params=pltpu.CompilerParams(collective_id=1, has_side_effects=True),
        name='collect_lent',
    )(mine)


GROUP = 4
BUFFERS = 4
PARTS = 2


def apply_kernel(shards, caps, skips, num_rows, *refs):
    lists = len(caps)
    rows, (lent, table), grads, out = refs[:lists], refs[lists:lists + 2], refs[lists + 2:2 * lists + 2], refs[2 * lists + 2]
    total, buf, load_sem, grad_sem, store_sem = refs[2 * lists + 3:]
    width = table.shape[1] // PARTS
    segments = [(part, i) for part in range(PARTS) for i in range(lists)]

    def columns(part):
        return pl.ds(part * width, width)

    def load(part):
        return pltpu.make_async_copy(table.at[:, columns(part)], total.at[pl.ds(0, num_rows), columns(part)], load_sem.at[part])

    def store(part):
        return pltpu.make_async_copy(total.at[pl.ds(0, num_rows), columns(part)], out.at[:, columns(part)], store_sem.at[part])

    def copy(segment, source):
        part, i = segment
        place = lax.rem(source, BUFFERS)
        return pltpu.make_async_copy(grads[i].at[source, :, columns(part)], buf.at[place, pl.ds(0, caps[i])], grad_sem.at[place])

    for part in range(PARTS):
        load(part).start()
    for source in range(BUFFERS - 1):
        copy(segments[0], source).start()
    for number, segment in enumerate(segments):
        part, i = segment
        if i == 0:
            load(part).wait()
            total[pl.ds(0, lent.shape[0]), columns(part)] += lent[:, columns(part)]

        def from_source(source, carry):
            ahead = source + BUFFERS - 1

            @pl.when(ahead < shards)
            def _():
                copy(segment, ahead).start()

            if number + 1 < len(segments):
                @pl.when(ahead >= shards)
                def _():
                    copy(segments[number + 1], ahead - shards).start()

            copy(segment, source).wait()
            place = lax.rem(source, BUFFERS)

            def group(step, carry):
                base = source * caps[i] + step * GROUP
                idx = [rows[i][base + k] for k in range(GROUP)]
                sums = [total[pl.ds(idx[k], 1), columns(part)] + buf[place, pl.ds(step * GROUP + k, 1), :] for k in range(GROUP)]
                for k in range(GROUP):
                    total[pl.ds(idx[k], 1), columns(part)] = sums[k]
                return carry

            return lax.fori_loop(skips[i] // GROUP, caps[i] // GROUP, group, carry)

        lax.fori_loop(0, shards, from_source, 0)
        if i == lists - 1:
            store(part).start()
    for part in range(PARTS):
        store(part).wait()


def apply_rows(table, lent, slots, grads, skips):
    num_rows, depth = table.shape
    shards = grads[0].shape[0]
    caps = tuple(g.shape[1] for g in grads)
    rows = [jnp.where(slot < TILE, num_rows, slot - TILE).reshape(-1) for slot in slots]
    any_space = pl.BlockSpec(memory_space=pl.ANY)
    moved = 2 * num_rows + sum(caps) * shards
    return pl.pallas_call(
        functools.partial(apply_kernel, shards, caps, skips, num_rows),
        out_shape=jax.ShapeDtypeStruct(table.shape, jnp.float32),
        in_specs=[pl.BlockSpec(memory_space=pltpu.SMEM)] * len(caps) + [pl.BlockSpec(memory_space=pltpu.VMEM), any_space] + [any_space] * len(caps),
        out_specs=any_space,
        scratch_shapes=[pltpu.VMEM((num_rows + TILE, depth), jnp.float32), pltpu.VMEM((BUFFERS, max(caps), depth // PARTS), jnp.float32), pltpu.SemaphoreType.DMA((PARTS,)), pltpu.SemaphoreType.DMA((BUFFERS,)), pltpu.SemaphoreType.DMA((PARTS,))],
        compiler_params=pltpu.CompilerParams(vmem_limit_bytes=40 * 2**20),
        cost_estimate=pl.CostEstimate(flops=40 * moved * depth, bytes_accessed=4 * moved * depth, transcendentals=0),
        name='apply_rows',
    )(*rows, lent, table, *grads)


def solution(mesh):
    shards = mesh.shape[AXIS_NAME]

    def device_step(in_shard, out_shard, center_ids, context_ids, negative_ids):
        shard_rows, depth = in_shard.shape
        num_negs = negative_ids.shape[0]
        lists = (center_ids, context_ids, negative_ids)
        full = tuple(up8(distinct_bound(ids.shape[0], shards) + TILE) for ids in lists)
        usual = tuple(up8(TILE + ids.shape[0] * 13 // (16 * shards)) for ids in lists)

        owners, ranks, asks, largest = zip(*(request_layout(ids, shard_rows, shards, cap) for ids, cap in zip(lists, full)))
        counts = jnp.broadcast_to(jnp.stack(largest)[None, :], (shards, 3))
        ask = jnp.concatenate(asks + (counts,), axis=1)
        ask = jnp.pad(ask, ((0, 0), (0, HEADER * LANES - ask.shape[1]))).reshape(shards, HEADER, LANES)
        arrived, lent_in, lent_out = ask_owners(ask, in_shard, out_shard, shards)
        arrived = arrived.reshape(shards, HEADER * LANES)
        edge1, edge2, edge3 = full[0], full[0] + full[1], sum(full)
        slots = (arrived[:, :edge1], arrived[:, edge1:edge2], arrived[:, edge2:edge3])
        most = jnp.max(arrived[:, edge3:edge3 + 3], axis=0)
        fits = jnp.all(most <= jnp.array(usual, jnp.int32))

        def onehot_f32(ids):
            return (ids[:, None] == lax.broadcasted_iota(jnp.int32, (1, shards * TILE), 1)).astype(jnp.float32)

        def lent_product(a, b, dims):
            return lax.dot_general(a, b, (dims, ((), ())), precision=lax.Precision.HIGHEST)

        def run(exchange, caps, in_shard, out_shard, lent_in, lent_out, context_ids, negative_ids, owners, ranks, slots):
            asked = [slot[:, :cap] for slot, cap in zip(slots, caps)]

            def pick(table, lent, slot):
                rows = take_rows(table, jnp.maximum(slot - TILE, 0))
                return lax.dynamic_update_slice(rows, jnp.broadcast_to(lent[None], (shards, TILE, depth)), (0, 0, 0))

            def send_back(start, cells, grads):
                summed = start.reshape(-1, depth).at[cells].add(grads, mode='drop')
                return exchange(summed.reshape(start.shape))

            in_cap, ctx_cap, neg_cap = caps
            in_cell = owners[0] * in_cap + ranks[0]
            ctx_cell = owners[1] * ctx_cap + ranks[1]
            ctx_cold = jnp.maximum(ctx_cell - TILE * (owners[1] + 1), 0)
            neg_cell = owners[2] * neg_cap + ranks[2]
            neg_cold = jnp.where(ranks[2] < TILE, shards * (neg_cap - TILE), neg_cell - TILE * (owners[2] + 1))

            picked = pick(out_shard, lent_out, asked[2])
            neg_rows, in_rows, ctx_blocks = fetch_rows(asked[0], asked[1][:, TILE:], picked, in_shard, out_shard, lent_in, 4 if caps == usual else 5)
            ctx_rows = exchange(ctx_blocks).reshape(-1, depth)

            negative_half = take_rows(neg_rows, neg_cell).astype(jnp.bfloat16)
            center_vec = take_rows(in_rows, in_cell)
            center_half = center_vec.astype(jnp.bfloat16)
            neg_score = dot_f32(center_half, negative_half, ((1,), (1,)))
            neg_grad = ((NEG_WEIGHT / num_negs) * jax.nn.sigmoid(neg_score)).astype(jnp.bfloat16)
            d_negative = -dot_f32(neg_grad, center_half, ((0,), (0,)))
            neg_back = send_back(jnp.zeros((shards, neg_cap - TILE, depth), jnp.float32), neg_cold, d_negative)
            d_center_neg = dot_f32(neg_grad, negative_half, ((1,), (0,)))
            lent_neg = lent_product(onehot_f32(negative_ids), d_negative, ((0,), (0,)))
            lent_rows = neg_rows.reshape(shards, neg_cap, depth)[:, :TILE].reshape(-1, depth)
            lent_ctx = lent_product(onehot_f32(context_ids), lent_rows, ((1,), (0,)))
            lent_ctx, d_center_neg = lax.optimization_barrier((lent_ctx, d_center_neg))

            context_vec = jnp.where((ranks[1] < TILE)[:, None], lent_ctx, take_rows(ctx_rows, ctx_cold))
            pos_grad = (jax.nn.sigmoid(jnp.sum(center_vec * context_vec, axis=1)) - 1.0)[:, None]
            start = jnp.pad(lent_neg.reshape(shards, TILE, depth), ((0, 0), (0, ctx_cap - TILE), (0, 0)))
            ctx_back = send_back(start, ctx_cell, -(pos_grad * center_vec))
            in_back = send_back(jnp.zeros((shards, in_cap, depth), jnp.float32), in_cell, -(pos_grad * context_vec + d_center_neg))

            new_out = apply_rows(out_shard, jnp.zeros((TILE, depth), jnp.float32), (asked[2][:, TILE:], asked[1]), (neg_back, ctx_back), (0, TILE))
            sums = [jnp.sum(back[:, :TILE], axis=0) for back in (in_back, ctx_back)]
            total = LEARN_RATE * collect_lent(jnp.concatenate(sums, axis=0), shards)
            new_in = apply_rows(in_shard, total[:, :TILE].reshape(-1, depth), (asked[0],), (in_back,), (TILE,))
            new_out = new_out.at[:shards * TILE].add(total[:, TILE:].reshape(-1, depth))
            return new_in, new_out

        def exchange_full(blocks):
            shapes = (full[0], full[1] - TILE, full[2] - TILE)
            return exchange_rows(blocks, (2, 3, 6)[shapes.index(blocks.shape[1])])

        def branch(swap, caps):
            def call(*args):
                return run(swap, caps, *args)

            return call

        args = (in_shard, out_shard, lent_in, lent_out, context_ids, negative_ids, owners, ranks, slots)
        return lax.cond(fits, branch(exchange, usual), branch(exchange_full, full), *args)

    return jax.shard_map(device_step, mesh=mesh, in_specs=(P(AXIS_NAME, None), P(AXIS_NAME, None), P(AXIS_NAME), P(AXIS_NAME), P(AXIS_NAME)), out_specs=(P(AXIS_NAME, None), P(AXIS_NAME, None)), check_vma=False)
```

```python
import functools

import jax
import jax.numpy as jnp
from jax import lax
from jax.experimental import pallas as pl
from jax.experimental.pallas import tpu as pltpu
from jax.sharding import PartitionSpec as P

LEARN_RATE = 1.0
NEG_WEIGHT = 5.0
AXIS_NAME = 'vp'
TILE = 8
LANES = 128
SLOT_BLOCKS = 16
HEADER = 8


def up8(count):
    return (count + 7) // 8 * 8


def distinct_bound(num_ids, shards):
    common_slots = 3 * num_ids // shards
    return common_slots // 4 + (num_ids - common_slots + shards - 1) // shards


def onehot(values, size):
    return (values[:, None] == lax.broadcasted_iota(jnp.int32, (1, size), 1)).astype(jnp.bfloat16)


def dot_f32(a, b, dims):
    return lax.dot_general(a, b, (dims, ((), ())), preferred_element_type=jnp.float32)


def request_layout(id_list, shard_rows, shards, capacity):
    hot = id_list < shards * TILE
    owner = jnp.where(hot, id_list // TILE, id_list // shard_rows)
    slot = jnp.where(hot, id_list % TILE, id_list % shard_rows + TILE)
    high = onehot(owner * SLOT_BLOCKS + slot // LANES, shards * SLOT_BLOCKS)
    low = onehot(slot % LANES, LANES)
    count = dot_f32(high, low, ((0,), (0,)))
    shape = (shards * SLOT_BLOCKS, LANES)
    row_idx = lax.broadcasted_iota(jnp.int32, shape, 0)
    lane_idx = lax.broadcasted_iota(jnp.int32, shape, 1)
    lent = (row_idx % SLOT_BLOCKS == 0) & (lane_idx < TILE)
    present = (count > 0.0) | lent
    ones = present.astype(jnp.bfloat16)
    upper = (lax.broadcasted_iota(jnp.int32, (LANES, LANES), 0) <= lax.broadcasted_iota(jnp.int32, (LANES, LANES), 1)).astype(jnp.bfloat16)
    inclusive = dot_f32(ones, upper, ((1,), (0,)))
    block_total = jnp.sum(present.astype(jnp.float32), axis=1).reshape(shards, SLOT_BLOCKS)
    before = (lax.broadcasted_iota(jnp.int32, (SLOT_BLOCKS, SLOT_BLOCKS), 0) < lax.broadcasted_iota(jnp.int32, (SLOT_BLOCKS, SLOT_BLOCKS), 1))
    block_start = dot_f32(block_total.astype(jnp.bfloat16), before.astype(jnp.bfloat16), ((1,), (0,)))
    rank = inclusive - ones.astype(jnp.float32) + block_start.reshape(-1)[:, None]
    rank_of_id = jnp.sum(dot_f32(high, rank.astype(jnp.bfloat16), ((1,), (0,))) * low.astype(jnp.float32), axis=1).astype(jnp.int32)
    rank_or_none = jnp.where(present, rank, -1.0).reshape(shards, 1, SLOT_BLOCKS * LANES)
    cells = lax.broadcasted_iota(jnp.int32, (1, capacity, 1), 1).astype(jnp.float32)
    slots = lax.broadcasted_iota(jnp.int32, (1, 1, SLOT_BLOCKS * LANES), 2).astype(jnp.float32)
    slot_of_cell = jnp.sum(jnp.where(rank_or_none == cells, slots + 1.0, 0.0), axis=2).astype(jnp.int32) - 1
    return owner, rank_of_id, slot_of_cell


def exchange(blocks):
    return lax.all_to_all(blocks, AXIS_NAME, 0, 0)


def take_rows(rows, idx):
    return rows.at[idx].get(mode='promise_in_bounds')


def meet(me, shards):
    barrier = pltpu.get_barrier_semaphore()
    for step in range(1, shards):
        pl.semaphore_signal(barrier, inc=1, device_id=(lax.rem(me + step, shards),), device_id_type=pl.DeviceIdType.MESH)
    pl.semaphore_wait(barrier, shards - 1)


def remote(src, dst, send_sem, recv_sem, peer):
    return pltpu.make_async_remote_copy(src_ref=src, dst_ref=dst, send_sem=send_sem, recv_sem=recv_sem, device_id=(peer,), device_id_type=pl.DeviceIdType.MESH)


def ask_kernel(shards, ask, got, send_sem, recv_sem):
    me = lax.axis_index(AXIS_NAME)
    meet(me, shards)
    copies = []
    for step in range(1, shards):
        peer = lax.rem(me + step, shards)
        copies.append(remote(ask.at[peer], got.at[me], send_sem.at[step], recv_sem.at[step], peer))
        copies[-1].start()
    got[me] = ask[me]
    for copy in copies:
        copy.wait()


def ask_owners(ask):
    shards = ask.shape[0]
    vmem = pl.BlockSpec(memory_space=pltpu.VMEM)
    return pl.pallas_call(
        functools.partial(ask_kernel, shards),
        out_shape=jax.ShapeDtypeStruct(ask.shape, jnp.int32),
        in_specs=[vmem],
        out_specs=vmem,
        scratch_shapes=[pltpu.SemaphoreType.DMA((shards,)), pltpu.SemaphoreType.DMA((shards,))],
        compiler_params=pltpu.CompilerParams(collective_id=0, has_side_effects=True),
        name='ask_owners',
    )(ask)


def exchange_kernel(shards, blocks, got, send_sem, recv_sem, own_sem):
    me = lax.axis_index(AXIS_NAME)
    meet(me, shards)
    own = pltpu.make_async_copy(blocks.at[me], got.at[me], own_sem)
    own.start()

    def copy(step, rows):
        peer = lax.rem(me + step, shards)
        return remote(blocks.at[peer, rows], got.at[me, rows], send_sem.at[step], recv_sem.at[step], peer)

    def send(tile, carry):
        for step in range(1, shards):
            copy(step, pl.ds(pl.multiple_of(tile * TILE, TILE), TILE)).start()
        return carry

    count = blocks.shape[1]
    lax.fori_loop(0, count // TILE, send, 0)
    for step in range(1, shards):
        copy(step, pl.ds(0, count)).wait()
    own.wait()


def exchange_rows(blocks, collective_id):
    shards = blocks.shape[0]
    any_space = pl.BlockSpec(memory_space=pl.ANY)
    return pl.pallas_call(
        functools.partial(exchange_kernel, shards),
        out_shape=jax.ShapeDtypeStruct(blocks.shape, jnp.float32),
        in_specs=[any_space],
        out_specs=any_space,
        scratch_shapes=[pltpu.SemaphoreType.DMA((shards,)), pltpu.SemaphoreType.DMA((shards,)), pltpu.SemaphoreType.DMA],
        compiler_params=pltpu.CompilerParams(collective_id=collective_id, has_side_effects=True),
    )(blocks)


def fetch_kernel(shards, in_idx, ctx_idx, neg_blocks, in_shard, out_shard, neg_got, in_got, in_blocks, ctx_blocks,
                 held, stage, lent, neg_send, neg_recv, in_send, in_recv, hot_send, hot_recv, lend_send, lend_recv, own_sem, load_sem, stage_sem):
    me = lax.axis_index(AXIS_NAME)
    load_in = pltpu.make_async_copy(in_shard, held, load_sem)
    load_in.start()
    meet(me, shards)

    def lend(part, peer):
        table = (in_shard, out_shard)[part]
        return remote(table.at[pl.ds(pl.multiple_of(peer * TILE, TILE), TILE)], lent.at[part], lend_send.at[part, peer], lend_recv.at[part], peer)

    def keep(part):
        return pltpu.make_async_copy((in_shard, out_shard)[part].at[pl.ds(0, TILE)], lent.at[part], own_sem.at[2 + part])

    @pl.when(me == 0)
    def _():
        for part in range(2):
            keep(part).start()
            for peer in range(1, shards):
                lend(part, peer).start()

    def exchange(blocks, got, send_sem, recv_sem):
        count = blocks.shape[1]

        def copy(step, first, rows):
            peer = lax.rem(me + step, shards)
            return remote(blocks.at[peer, pl.ds(first, rows)], got.at[me, pl.ds(first + TILE, rows)], send_sem.at[step], recv_sem.at[step], peer)

        def send(tile, carry):
            for step in range(1, shards):
                copy(step, pl.multiple_of(tile * TILE, TILE), TILE).start()
            return carry

        def finish():
            for step in range(1, shards):
                copy(step, 0, count).wait()

        lax.fori_loop(0, count // TILE, send, 0)
        return finish

    def pick(idx, blocks):
        count = blocks.shape[1]

        def put(peer, place):
            return pltpu.make_async_copy(stage.at[place, pl.ds(0, count)], blocks.at[peer], stage_sem.at[place])

        def for_peer(peer, carry):
            place = lax.rem(peer, 2)

            @pl.when(peer >= 2)
            def _():
                put(peer - 2, place).wait()

            def group(step, carry):
                first = step * TILE
                for k in range(TILE):
                    stage[place, pl.ds(first + k, 1), :] = held[pl.ds(idx[peer * count + first + k], 1), :]
                return carry

            lax.fori_loop(0, count // TILE, group, 0)
            put(peer, place).start()
            return carry

        lax.fori_loop(0, shards, for_peer, 0)
        put(shards - 2, 0).wait()
        put(shards - 1, 1).wait()

    finish_neg = exchange(neg_blocks, neg_got, neg_send, neg_recv)
    own_neg = pltpu.make_async_copy(neg_blocks.at[me], neg_got.at[me, pl.ds(TILE, neg_blocks.shape[1])], own_sem.at[0])
    own_neg.start()
    load_in.wait()
    pick(in_idx, in_blocks)

    @pl.when(me == 0)
    def _():
        for part in range(2):
            keep(part).wait()
            for peer in range(1, shards):
                lend(part, peer).wait_send()

    @pl.when(me != 0)
    def _():
        for part in range(2):
            lend(part, me).wait_recv()

    hot = []
    for part, got in enumerate((in_got, neg_got)):
        hot.append(pltpu.make_async_copy(lent.at[part], got.at[me, pl.ds(0, TILE)], own_sem.at[4 + part]))
        for step in range(1, shards):
            hot.append(remote(lent.at[part], got.at[me, pl.ds(0, TILE)], hot_send.at[part, step], hot_recv.at[part, step], lax.rem(me + step, shards)))
    for copy in hot:
        copy.start()
    finish_in = exchange(in_blocks, in_got, in_send, in_recv)
    own_in = pltpu.make_async_copy(in_blocks.at[me], in_got.at[me, pl.ds(TILE, in_blocks.shape[1])], own_sem.at[1])
    own_in.start()
    load_out = pltpu.make_async_copy(out_shard, held, load_sem)
    load_out.start()
    load_out.wait()
    pick(ctx_idx, ctx_blocks)
    own_neg.wait()
    own_in.wait()
    finish_neg()
    for copy in hot:
        copy.wait()
    finish_in()


def fetch_rows(in_slot, ctx_slot, neg_blocks, in_shard, out_shard, collective_id):
    shards, in_cap = in_slot.shape
    ctx_cap, depth = ctx_slot.shape[1], in_shard.shape[1]
    smem, any_space = pl.BlockSpec(memory_space=pltpu.SMEM), pl.BlockSpec(memory_space=pl.ANY)

    def rows(count):
        return jax.ShapeDtypeStruct((shards, count, depth), jnp.float32)

    def sems(*shape):
        return pltpu.SemaphoreType.DMA(shape)

    neg_got, in_got, _, ctx_blocks = pl.pallas_call(
        functools.partial(fetch_kernel, shards),
        out_shape=(rows(neg_blocks.shape[1] + TILE), rows(in_cap + TILE), rows(in_cap), rows(ctx_cap)),
        in_specs=[smem, smem, any_space, any_space, any_space],
        out_specs=(any_space,) * 4,
        scratch_shapes=[pltpu.VMEM(in_shard.shape, jnp.float32), pltpu.VMEM((2, max(in_cap, ctx_cap), depth), jnp.float32), pltpu.VMEM((2, TILE, depth), jnp.float32)]
        + [sems(shards)] * 4 + [sems(2, shards)] * 3 + [sems(2), sems(6), pltpu.SemaphoreType.DMA, sems(2)],
        compiler_params=pltpu.CompilerParams(collective_id=collective_id, has_side_effects=True, vmem_limit_bytes=40 * 2**20),
    )(jnp.maximum(in_slot - TILE, 0).reshape(-1), jnp.maximum(ctx_slot - TILE, 0).reshape(-1), neg_blocks, in_shard, out_shard)
    return neg_got.reshape(-1, depth), in_got.reshape(-1, depth), ctx_blocks


def collect_kernel(shards, mine, got, send_sem, recv_sem):
    me = lax.axis_index(AXIS_NAME)
    ready = pltpu.get_barrier_semaphore()

    @pl.when(me == 0)
    def _():
        for peer in range(1, shards):
            pl.semaphore_signal(ready, inc=1, device_id=(peer,), device_id_type=pl.DeviceIdType.MESH)
        got[0] = mine[...]
        for peer in range(1, shards):
            remote(mine, got.at[peer], send_sem, recv_sem.at[peer], 0).wait_recv()

    @pl.when(me != 0)
    def _():
        pl.semaphore_wait(ready, 1)
        got[...] = jnp.zeros_like(got)
        copy = remote(mine, got.at[me], send_sem, recv_sem.at[me], 0)
        copy.start()
        copy.wait_send()


def collect_lent(mine, shards):
    vmem = pl.BlockSpec(memory_space=pltpu.VMEM)
    return pl.pallas_call(
        functools.partial(collect_kernel, shards),
        out_shape=jax.ShapeDtypeStruct((shards,) + mine.shape, jnp.float32),
        in_specs=[vmem],
        out_specs=vmem,
        scratch_shapes=[pltpu.SemaphoreType.DMA, pltpu.SemaphoreType.DMA((shards,))],
        compiler_params=pltpu.CompilerParams(collective_id=1, has_side_effects=True),
        name='collect_lent',
    )(mine)


GROUP = 4
BUFFERS = 4
PARTS = 2


def apply_kernel(shards, caps, skips, num_rows, *refs):
    lists = len(caps)
    rows, (lent, table), grads, out = refs[:lists], refs[lists:lists + 2], refs[lists + 2:2 * lists + 2], refs[2 * lists + 2]
    total, buf, load_sem, grad_sem, store_sem = refs[2 * lists + 3:]
    width = table.shape[1] // PARTS
    segments = [(part, i) for part in range(PARTS) for i in range(lists)]

    def columns(part):
        return pl.ds(part * width, width)

    def load(part):
        return pltpu.make_async_copy(table.at[:, columns(part)], total.at[pl.ds(0, num_rows), columns(part)], load_sem.at[part])

    def store(part):
        return pltpu.make_async_copy(total.at[pl.ds(0, num_rows), columns(part)], out.at[:, columns(part)], store_sem.at[part])

    def copy(segment, source):
        part, i = segment
        place = lax.rem(source, BUFFERS)
        return pltpu.make_async_copy(grads[i].at[source, :, columns(part)], buf.at[place, pl.ds(0, caps[i])], grad_sem.at[place])

    for part in range(PARTS):
        load(part).start()
    for source in range(BUFFERS - 1):
        copy(segments[0], source).start()
    for number, segment in enumerate(segments):
        part, i = segment
        if i == 0:
            load(part).wait()
            total[pl.ds(0, lent.shape[0]), columns(part)] += lent[:, columns(part)]

        def from_source(source, carry):
            ahead = source + BUFFERS - 1

            @pl.when(ahead < shards)
            def _():
                copy(segment, ahead).start()

            if number + 1 < len(segments):
                @pl.when(ahead >= shards)
                def _():
                    copy(segments[number + 1], ahead - shards).start()

            copy(segment, source).wait()
            place = lax.rem(source, BUFFERS)

            def group(step, carry):
                base = source * caps[i] + step * GROUP
                idx = [rows[i][base + k] for k in range(GROUP)]
                sums = [total[pl.ds(idx[k], 1), columns(part)] + buf[place, pl.ds(step * GROUP + k, 1), :] for k in range(GROUP)]
                for k in range(GROUP):
                    total[pl.ds(idx[k], 1), columns(part)] = sums[k]
                return carry

            return lax.fori_loop(skips[i] // GROUP, caps[i] // GROUP, group, carry)

        lax.fori_loop(0, shards, from_source, 0)
        if i == lists - 1:
            store(part).start()
    for part in range(PARTS):
        store(part).wait()


def apply_rows(table, lent, slots, grads, skips):
    num_rows, depth = table.shape
    shards = grads[0].shape[0]
    caps = tuple(g.shape[1] for g in grads)
    rows = [jnp.where(slot < TILE, num_rows, slot - TILE).reshape(-1) for slot in slots]
    any_space = pl.BlockSpec(memory_space=pl.ANY)
    moved = 2 * num_rows + sum(caps) * shards
    return pl.pallas_call(
        functools.partial(apply_kernel, shards, caps, skips, num_rows),
        out_shape=jax.ShapeDtypeStruct(table.shape, jnp.float32),
        in_specs=[pl.BlockSpec(memory_space=pltpu.SMEM)] * len(caps) + [pl.BlockSpec(memory_space=pltpu.VMEM), any_space] + [any_space] * len(caps),
        out_specs=any_space,
        scratch_shapes=[pltpu.VMEM((num_rows + TILE, depth), jnp.float32), pltpu.VMEM((BUFFERS, max(caps), depth // PARTS), jnp.float32), pltpu.SemaphoreType.DMA((PARTS,)), pltpu.SemaphoreType.DMA((BUFFERS,)), pltpu.SemaphoreType.DMA((PARTS,))],
        compiler_params=pltpu.CompilerParams(vmem_limit_bytes=40 * 2**20),
        cost_estimate=pl.CostEstimate(flops=40 * moved * depth, bytes_accessed=4 * moved * depth, transcendentals=0),
        name='apply_rows',
    )(*rows, lent, table, *grads)


def solution(mesh):
    shards = mesh.shape[AXIS_NAME]

    def device_step(in_shard, out_shard, center_ids, context_ids, negative_ids):
        shard_rows, depth = in_shard.shape
        num_negs = negative_ids.shape[0]
        lists = (center_ids, context_ids, negative_ids)
        full = tuple(up8(distinct_bound(ids.shape[0], shards) + TILE) for ids in lists)
        usual = tuple(up8(TILE + ids.shape[0] * 13 // (16 * shards)) for ids in lists)

        owners, ranks, asks = zip(*(request_layout(ids, shard_rows, shards, cap) for ids, cap in zip(lists, full)))
        beyond = jnp.concatenate([ask[:, cap:cap + 1] for ask, cap in zip(asks, usual)], axis=1)
        over = jnp.broadcast_to(jnp.max(beyond), (shards, 1))
        ask = jnp.concatenate(asks + (over,), axis=1)
        ask = jnp.pad(ask, ((0, 0), (0, HEADER * LANES - ask.shape[1]))).reshape(shards, HEADER, LANES)
        arrived = ask_owners(ask)
        arrived = arrived.reshape(shards, HEADER * LANES)
        edge1, edge2, edge3 = full[0], full[0] + full[1], sum(full)
        slots = (arrived[:, :edge1], arrived[:, edge1:edge2], arrived[:, edge2:edge3])
        fits = jnp.max(arrived[:, edge3]) < 0

        def onehot_f32(ids):
            return (ids[:, None] == lax.broadcasted_iota(jnp.int32, (1, shards * TILE), 1)).astype(jnp.float32)

        def lent_product(a, b, dims):
            return lax.dot_general(a, b, (dims, ((), ())), precision=lax.Precision.HIGHEST)

        def run(exchange, caps, in_shard, out_shard, context_ids, negative_ids, owners, ranks, slots):
            asked = [slot[:, :cap] for slot, cap in zip(slots, caps)]

            def send_back(start, cells, grads):
                summed = start.reshape(-1, depth).at[cells].add(grads, mode='drop')
                return exchange(summed.reshape(start.shape))

            in_cap, ctx_cap, neg_cap = caps
            in_cell = owners[0] * in_cap + ranks[0]
            ctx_cell = owners[1] * ctx_cap + ranks[1]
            ctx_cold = jnp.maximum(ctx_cell - TILE * (owners[1] + 1), 0)
            neg_cell = owners[2] * neg_cap + ranks[2]
            neg_cold = jnp.where(ranks[2] < TILE, shards * (neg_cap - TILE), neg_cell - TILE * (owners[2] + 1))

            picked = take_rows(out_shard, jnp.maximum(asked[2][:, TILE:] - TILE, 0))
            neg_rows, in_rows, ctx_blocks = fetch_rows(asked[0][:, TILE:], asked[1][:, TILE:], picked, in_shard, out_shard, 4 if caps == usual else 5)
            ctx_rows = exchange(ctx_blocks).reshape(-1, depth)

            negative_half = take_rows(neg_rows, neg_cell).astype(jnp.bfloat16)
            center_vec = take_rows(in_rows, in_cell)
            center_half = center_vec.astype(jnp.bfloat16)
            neg_score = dot_f32(center_half, negative_half, ((1,), (1,)))
            neg_grad = ((NEG_WEIGHT / num_negs) * jax.nn.sigmoid(neg_score)).astype(jnp.bfloat16)
            d_negative = -dot_f32(neg_grad, center_half, ((0,), (0,)))
            neg_back = send_back(jnp.zeros((shards, neg_cap - TILE, depth), jnp.float32), neg_cold, d_negative)
            d_center_neg = dot_f32(neg_grad, negative_half, ((1,), (0,)))
            lent_neg = lent_product(onehot_f32(negative_ids), d_negative, ((0,), (0,)))
            lent_rows = neg_rows.reshape(shards, neg_cap, depth)[:, :TILE].reshape(-1, depth)
            lent_ctx = lent_product(onehot_f32(context_ids), lent_rows, ((1,), (0,)))
            lent_ctx, d_center_neg = lax.optimization_barrier((lent_ctx, d_center_neg))

            context_vec = jnp.where((ranks[1] < TILE)[:, None], lent_ctx, take_rows(ctx_rows, ctx_cold))
            pos_grad = (jax.nn.sigmoid(jnp.sum(center_vec * context_vec, axis=1)) - 1.0)[:, None]
            start = jnp.pad(lent_neg.reshape(shards, TILE, depth), ((0, 0), (0, ctx_cap - TILE), (0, 0)))
            ctx_back = send_back(start, ctx_cell, -(pos_grad * center_vec))
            in_back = send_back(jnp.zeros((shards, in_cap, depth), jnp.float32), in_cell, -(pos_grad * context_vec + d_center_neg))

            new_out = apply_rows(out_shard, jnp.zeros((TILE, depth), jnp.float32), (asked[2][:, TILE:], asked[1]), (neg_back, ctx_back), (0, TILE))
            sums = [jnp.sum(back[:, :TILE], axis=0) for back in (in_back, ctx_back)]
            total = LEARN_RATE * collect_lent(jnp.concatenate(sums, axis=0), shards)
            new_in = apply_rows(in_shard, total[:, :TILE].reshape(-1, depth), (asked[0],), (in_back,), (TILE,))
            new_out = new_out.at[:shards * TILE].add(total[:, TILE:].reshape(-1, depth))
            return new_in, new_out

        def exchange_full(blocks):
            shapes = (full[0], full[1] - TILE, full[2] - TILE)
            return exchange_rows(blocks, (2, 3, 6)[shapes.index(blocks.shape[1])])

        def branch(swap, caps):
            def call(*args):
                return run(swap, caps, *args)

            return call

        args = (in_shard, out_shard, context_ids, negative_ids, owners, ranks, slots)
        return lax.cond(fits, branch(exchange, usual), branch(exchange_full, full), *args)

    return jax.shard_map(device_step, mesh=mesh, in_specs=(P(AXIS_NAME, None), P(AXIS_NAME, None), P(AXIS_NAME), P(AXIS_NAME), P(AXIS_NAME)), out_specs=(P(AXIS_NAME, None), P(AXIS_NAME, None)), check_vma=False)
```
